32 devices in a mesh: space: 2 (over x), energy: 16 (over z, y, core).
Axes of the slice: x: 2, y: 2, z: 4, core: 2. Of those that a mesh axis runs over, the one named last changes fastest.
Arguments:
- lesser_in: bfloat16 [16, 2, 2, 256, 256], P('energy', 'space'), may hold values from -6 to 6
- retarded: bfloat16 [16, 2, 2, 256, 256], P('energy', 'space'), may hold values from -0.25 to 0.25
- coupling: bfloat16 [2, 2, 256, 256], P('space'), may hold values from -0.25 to 0.25
- interaction: bfloat16 [2, 32, 65536], P('space', None, 'energy'), may hold values from -1.5 to 1.5
Outputs:
- self_energy: bfloat16 [16, 2, 2, 256, 256], P('energy', 'space')
The draws below stay inside these ranges and needn't reach their ends.
All inputs are finite; a program needn't handle non-finite values.
Results may differ from the reference program's by a relative error of at most 0.029.
Values may be sent and summed in bfloat16 or wider, within the bound.
A program may use at most 128 MiB of HBM per device.

```python
import math
import jax
import jax.numpy as jnp
from jax import lax

B = 256
NBLK = 2
NE = 16
NFFT = 32


def level_of(stream_key, extent, split, low, high):
    gain, own = 1.0, jax.random.fold_in(stream_key, 6)
    for axis_at, parts in split:
        heights = jnp.exp(jax.random.uniform(jax.random.fold_in(own, axis_at), (parts,), jnp.float32, low / len(split), high / len(split)))
        gain = gain * jnp.repeat(heights, extent[axis_at] // parts).reshape([-1 if axis == axis_at else 1 for axis in range(len(extent))])
    return gain


def normal_values(key, extent, width, reach, shards=(), kind=jnp.bfloat16):
    values = jax.random.normal(key, extent, jnp.float32) * width
    if len(shards) > 0:
        values = level_of(key, extent, shards, -0.22, 0.18) * values
    return jnp.clip(values, min=-reach, max=reach).astype(kind)


def setup_inputs(seed: int = 0) -> dict:
    key_list = jax.random.split(jax.random.key(seed), 5)
    lesser_in = normal_values(key_list[0], (NE, NBLK, 2, B, B), 1.0, 6.0, ((0, 16), (1, 2)))
    retarded = normal_values(key_list[1], (NE, NBLK, 2, B, B), (2 * B) ** -0.5, 0.25, ((0, 16), (1, 2)))
    coupling = normal_values(key_list[2], (NBLK, 2, B, B), (2 * B + B // 3) ** -0.5, 0.25, ((0, 2),))
    interaction = normal_values(key_list[3], (NBLK, NFFT, B * B), 0.25, 1.5, ((0, 2), (2, 16)))
    return dict(lesser_in=lesser_in, retarded=retarded, coupling=coupling, interaction=interaction)


def product(left_real, left_imag, right_real, right_imag):
    real_part = jnp.dot(left_real, right_real, preferred_element_type=jnp.float32) - jnp.dot(left_imag, right_imag, preferred_element_type=jnp.float32)
    imag_part = jnp.dot(left_real, right_imag, preferred_element_type=jnp.float32) + jnp.dot(left_imag, right_real, preferred_element_type=jnp.float32)
    return real_part, imag_part


def contract(former, latter):
    return lax.dot_general(former, latter, (((1,), (1,)), ((), ())), preferred_element_type=jnp.float32)


def product_adjoint(left_real, left_imag, right_real, right_imag):
    real_part = contract(left_real, right_real) + contract(left_imag, right_imag)
    imag_part = contract(left_imag, right_real) - contract(left_real, right_imag)
    return real_part, imag_part


def phase_table(row_count, column_count, length):
    row_index = jnp.arange(row_count, dtype=jnp.int32)[:, None]
    column_index = jnp.arange(column_count, dtype=jnp.int32)[None, :]
    residue = (row_index * column_index) % length
    return residue.astype(jnp.float32) * (2.0 * math.pi / length)


def finish(spectrum_real, spectrum_imag, weights, energy_count, length):
    forward_scale = energy_count ** -0.5
    inverse_scale = length ** -0.5
    spectrum_real = spectrum_real * forward_scale
    spectrum_imag = spectrum_imag * forward_scale
    weight_values = weights.astype(jnp.float32)
    squared_real = ((spectrum_real * spectrum_real - spectrum_imag * spectrum_imag) * weight_values).astype(jnp.bfloat16)
    squared_imag = (2.0 * spectrum_real * spectrum_imag * weight_values).astype(jnp.bfloat16)
    inverse_phase = phase_table(energy_count, length, length)
    inverse_real = jnp.cos(inverse_phase).astype(jnp.bfloat16)
    inverse_imag = jnp.sin(inverse_phase).astype(jnp.bfloat16)
    out_real, out_imag = product(inverse_real, inverse_imag, squared_real, squared_imag)
    return jnp.stack([out_real * inverse_scale, out_imag * inverse_scale], axis=1).astype(jnp.bfloat16)


def reference(lesser_in, retarded, coupling, interaction):
    block_order = coupling.shape[-1]
    block_count = coupling.shape[0]
    energy_count = lesser_in.shape[0]
    length = 2 * energy_count

    def one_energy(inputs_pair):
        green_in, lesser_here = inputs_pair
        carried_real = jnp.zeros((block_order, block_order), jnp.bfloat16)
        carried_imag = jnp.zeros((block_order, block_order), jnp.bfloat16)
        layers = []
        for block_index in range(block_count):
            resolvent_real = green_in[block_index, 0]
            resolvent_imag = green_in[block_index, 1]
            map_real, map_imag = product(resolvent_real, resolvent_imag, coupling[block_index, 0], coupling[block_index, 1])
            map_real = map_real.astype(jnp.bfloat16)
            map_imag = map_imag.astype(jnp.bfloat16)
            half_real, half_imag = product(resolvent_real, resolvent_imag, lesser_here[block_index, 0], lesser_here[block_index, 1])
            half_real = half_real.astype(jnp.bfloat16)
            half_imag = half_imag.astype(jnp.bfloat16)
            source_real, source_imag = product_adjoint(half_real, half_imag, resolvent_real, resolvent_imag)
            carry_real, carry_imag = product(map_real, map_imag, carried_real, carried_imag)
            carry_real = carry_real.astype(jnp.bfloat16)
            carry_imag = carry_imag.astype(jnp.bfloat16)
            grown_real, grown_imag = product_adjoint(carry_real, carry_imag, map_real, map_imag)
            carried_real = (source_real + grown_real).astype(jnp.bfloat16)
            carried_imag = (source_imag + grown_imag).astype(jnp.bfloat16)
            layers.append(jnp.stack([carried_real, carried_imag]))
        return jnp.stack(layers)

    green_lesser = lax.map(one_energy, (retarded, lesser_in))
    forward_phase = phase_table(length, energy_count, length)
    forward_real = jnp.cos(forward_phase).astype(jnp.bfloat16)
    forward_imag = (-jnp.sin(forward_phase)).astype(jnp.bfloat16)

    def one_block(inputs_pair):
        green_block, weights = inputs_pair
        flattened = green_block.reshape(energy_count, 2, block_order * block_order)
        spectrum_real, spectrum_imag = product(forward_real, forward_imag, flattened[:, 0], flattened[:, 1])
        result = finish(spectrum_real, spectrum_imag, weights, energy_count, length)
        return result.reshape(energy_count, 2, block_order, block_order)

    per_block = lax.map(one_block, (jnp.moveaxis(green_lesser, 1, 0), interaction))
    return jnp.moveaxis(per_block, 0, 1)
```

```python
import functools
import math

import jax
import jax.numpy as jnp
import numpy as np
from jax import lax
from jax.experimental import pallas as pl
from jax.experimental.pallas import tpu as pltpu
from jax.sharding import PartitionSpec as P

MESH = pl.DeviceIdType.MESH
ANY = pl.BlockSpec(memory_space=pl.ANY)
LOW, WIDE = jnp.bfloat16, jnp.float32


def phase_parts(row_count, column_count, length):
    residue = np.arange(row_count)[:, None] * np.arange(column_count)[None, :] % length
    phase = residue * (2.0 * math.pi / length)
    return np.cos(phase), np.sin(phase)


def forward_matrix(energies, length, rows):
    cosine, sine = phase_parts(length, max(energies) + 1, length)
    cosine, sine = cosine[:, energies], sine[:, energies]
    small = np.array([[cosine, sine], [-sine, cosine]])
    full = np.einsum("pqfe,rs->rpfeqs", small, np.eye(rows))
    return full.reshape(rows * 2 * length, len(energies) * 2 * rows).astype(LOW)


def inverse_matrix(energy_count, length, rows):
    cosine, sine = phase_parts(energy_count, length, length)
    small = np.array([[cosine, -sine], [sine, cosine]])
    full = np.einsum("pqef,rs->eprsqf", small, np.eye(rows))
    return full.reshape(energy_count * 2 * rows, rows * 2 * length).astype(LOW)


def dot(left, right):
    return jnp.dot(left, right, preferred_element_type=WIDE)


def dot_t(left, right):
    return lax.dot_general(left, right, (((1,), (1,)), ((), ())), preferred_element_type=WIDE)


def product(a_re, a_im, b_re, b_im):
    return dot(a_re, b_re) + dot(-a_im, b_im), dot(a_re, b_im) + dot(a_im, b_re)


def product_adjoint(a_re, a_im, b_re, b_im):
    return dot_t(a_re, b_re) + dot_t(a_im, b_im), dot_t(a_im, b_re) + dot_t(-a_re, b_im)


def flipped(index, mask):
    bit = 1
    while bit <= mask:
        if mask & bit:
            index = index + bit - 2 * bit * (index // bit % 2)
        bit *= 2
    return index


def kernel(
    sections, groups, rows, length, pieces, parts,
    lesser_hbm, retarded_hbm, coupling_hbm, interaction_hbm, forward_hbm, inverse_hbm,
    landed,
    lesser, retarded, coupling, interaction, forward, inverse,
    total, maps, green, before, theirs, carried, homing, homed, grown, weighted, leaving,
    load_sem, hop_send, hop_recv, map_send, map_recv, go_send, go_recv, late_send, late_recv,
    back_send, back_recv, own_sem,
):
    section = lax.axis_index("space")
    me = lax.axis_index("energy")
    order = green.shape[-1]
    width = order // pieces
    last = sections - 1
    split = sections > 1 and groups % 2 == 0
    half = groups // 2 if split else 0
    odd = me % 2 == 1 if split else me < 0
    is_last = section == last
    feeds = (section < last - 1) | ((section == last - 1) & ~odd)
    fed = (section > 0) & ((section < last) | ~odd)
    lends = is_last & odd & (section > 0)
    grows = (section == last - 1) & odd

    if groups & (groups - 1) == 0:
        peers = [flipped(me, mask) for mask in range(groups - 1, 0, -1)]
    else:
        peers = [lax.rem(me + step, groups) for step in range(1, groups)]

    barrier = pltpu.get_barrier_semaphore()
    for peer in peers:
        pl.semaphore_signal(barrier, inc=1, device_id={"energy": peer}, device_id_type=MESH)

    @pl.when(fed)
    def _():
        pl.semaphore_signal(barrier, inc=1, device_id={"space": section - 1}, device_id_type=MESH)

    if split:
        @pl.when(grows)
        def _():
            pl.semaphore_signal(barrier, inc=1, device_id={"space": last}, device_id_type=MESH)

        @pl.when(is_last)
        def _():
            for at in range(half):
                pl.semaphore_signal(
                    barrier, inc=1,
                    device_id={"space": last - 1, "energy": 2 * at + 1}, device_id_type=MESH,
                )

    loads = []
    for at, (source, target) in enumerate((
        (retarded_hbm.at[0, 0], retarded),
        (lesser_hbm.at[0, 0], lesser),
        (coupling_hbm.at[0], coupling),
        (interaction_hbm.at[0], interaction),
        (forward_hbm, forward),
        (inverse_hbm, inverse),
    )):
        load = pltpu.make_async_copy(source, target, load_sem.at[at])
        loads.append(load)
        if target is coupling:
            pl.when(section > 0)(load.start)
        else:
            load.start()

    def arrived():
        pl.semaphore_wait(
            barrier,
            groups - 1 + jnp.where(feeds, 1, 0) + jnp.where(lends, 1, 0)
            + jnp.where(grows, groups, 0),
        )

    def hop(piece):
        columns = pl.ds(piece * width, width)
        return pltpu.make_async_remote_copy(
            src_ref=green.at[:, :, columns],
            dst_ref=before.at[:, :, columns],
            send_sem=hop_send.at[piece],
            recv_sem=hop_recv.at[piece],
            device_id={"space": section + 1},
            device_id_type=MESH,
        )

    def lend(piece):
        lines = pl.ds(piece * width, width)
        return pltpu.make_async_remote_copy(
            src_ref=maps.at[:, lines, :],
            dst_ref=theirs.at[:, lines, :],
            send_sem=map_send.at[piece],
            recv_sem=map_recv.at[piece],
            device_id={"space": section - 1},
            device_id_type=MESH,
        )

    def make_maps():
        loads[2].wait()
        m_re, m_im = product(retarded[0], retarded[1], coupling[0], coupling[1])
        maps[0], maps[1] = m_re.astype(LOW), m_im.astype(LOW)

    loads[0].wait()

    @pl.when(lends)
    def _():
        make_maps()
        arrived()
        for piece in range(pieces):
            lend(piece).start()

    loads[1].wait()
    r_re, r_im = retarded[0], retarded[1]
    half_re, half_im = product(r_re, r_im, lesser[0], lesser[1])
    half_re, half_im = half_re.astype(LOW), half_im.astype(LOW)
    total[0], total[1] = product_adjoint(half_re, half_im, r_re, r_im)

    @pl.when(~lends)
    def _():
        arrived()

    @pl.when(fed)
    def _():
        make_maps()
        for piece in range(pieces):
            hop(piece).wait_recv()
            part = slice(piece * width, (piece + 1) * width)
            k_re, k_im = product(maps[0], maps[1], before[0, :, part], before[1, :, part])
            g_re, g_im = product_adjoint(
                k_re.astype(LOW), k_im.astype(LOW), maps[0, :, part], maps[1, :, part]
            )
            total[0] += g_re
            total[1] += g_im

    @pl.when(feeds | grows)
    def _():
        green[...] = total[...].astype(LOW)

    @pl.when(feeds)
    def _():
        for piece in range(pieces):
            hop(piece).start()

    share = rows // parts

    def scattered(values, target):
        for part in range(parts):
            target[part] = jnp.concatenate(
                [values[side].reshape(groups, parts, share, order)[:, part] for side in range(2)],
                axis=1,
            ).astype(LOW).reshape(groups, 2 * share, order)

    def go(part, peer, slot):
        return pltpu.make_async_remote_copy(
            src_ref=homing.at[part, peer],
            dst_ref=homed.at[part, slot],
            send_sem=go_send.at[part, peer],
            recv_sem=go_recv.at[part, slot],
            device_id={"energy": peer},
            device_id_type=MESH,
        )

    def late(part, peer, slot):
        return pltpu.make_async_remote_copy(
            src_ref=grown.at[part, peer],
            dst_ref=homed.at[part, groups + slot],
            send_sem=late_send.at[part, peer],
            recv_sem=late_recv.at[part, slot],
            device_id={"space": last, "energy": peer},
            device_id_type=MESH,
        )

    def back(part, peer, slot):
        return pltpu.make_async_remote_copy(
            src_ref=leaving.at[part, peer],
            dst_ref=landed.at[slot, part],
            send_sem=back_send.at[part, peer],
            recv_sem=back_recv.at[part, slot],
            device_id={"energy": peer},
            device_id_type=MESH,
        )

    scattered((total[0], total[1]), homing)
    kept = []
    for part in range(parts):
        for peer in peers:
            go(part, peer, me).start()
        own = pltpu.make_async_copy(homing.at[part, me], homed.at[part, me], own_sem.at[0, part])
        own.start()
        kept.append(own)

    if split:
        @pl.when(grows)
        def _():
            for piece in range(pieces):
                lend(piece).wait_recv()
                part = slice(piece * width, (piece + 1) * width)
                k_re, k_im = product(theirs[0, part, :], theirs[1, part, :], green[0], green[1])
                carried[0, part, :], carried[1, part, :] = k_re.astype(LOW), k_im.astype(LOW)
            g_re, g_im = product_adjoint(carried[0], carried[1], theirs[0], theirs[1])
            scattered((g_re, g_im), grown)
            for part in range(parts):
                for peer in peers + [me]:
                    late(part, peer, me // 2).start()

        @pl.when(~is_last)
        def _():
            for part in range(parts):
                homed[part, groups:] = jnp.zeros((half, 2 * share, order), LOW)

    for load in loads[3:]:
        load.wait()

    stride = 2 * length
    chunk = max(1, order // stride)
    returns = []
    for part in range(parts):
        kept[part].wait()
        for peer in peers:
            go(part, peer, peer).wait_recv()
        if split:
            @pl.when(is_last)
            def _():
                for at in range(half):
                    late(part, me, at).wait_recv()
        entries = homed[part]
        if 2 * share % 16:
            entries = entries.astype(WIDE)
        entries = entries.reshape((groups + half) * 2 * share, order).astype(LOW)
        for first in range(0, share, chunk):
            spectrum = dot(forward[first * stride:(first + chunk) * stride, :], entries)
            spectrum = spectrum * groups ** -0.5
            for at in range(chunk):
                row = first + at
                s_re = spectrum[at * stride:at * stride + length]
                s_im = spectrum[at * stride + length:(at + 1) * stride]
                entry = (part * share + row) * order
                weight = interaction[:, entry:entry + order].astype(WIDE)
                weighted[row * stride:row * stride + length, :] = (
                    (s_re * s_re - s_im * s_im) * weight
                ).astype(LOW)
                weighted[row * stride + length:(row + 1) * stride, :] = (
                    2.0 * s_re * s_im * weight
                ).astype(LOW)
        result = dot(inverse[...], weighted[...]) * length ** -0.5
        leaving[part] = result.reshape(groups, 2, share, order).astype(LOW)
        for peer in peers:
            back(part, peer, me).start()
        own = pltpu.make_async_copy(leaving.at[part, me], landed.at[me, part], own_sem.at[1, part])
        own.start()
        returns.append(own)

    for part in range(parts):
        for peer in peers:
            go(part, peer, me).wait_send()

    @pl.when(feeds)
    def _():
        for piece in range(pieces):
            hop(piece).wait_send()

    if split:
        @pl.when(lends)
        def _():
            for piece in range(pieces):
                lend(piece).wait_send()

        @pl.when(grows)
        def _():
            for part in range(parts):
                for peer in peers + [me]:
                    late(part, peer, me // 2).wait_send()

    for part in range(parts):
        returns[part].wait()
        for peer in peers:
            back(part, peer, me).wait_send()
        for peer in peers:
            back(part, peer, peer).wait_recv()


def write(parts, landed, out_hbm, sem):
    copies = []
    for part in range(parts):
        for side in range(2):
            copy = pltpu.make_async_copy(
                landed.at[:, part, side], out_hbm.at[side, :, part], sem.at[part, side]
            )
            copy.start()
            copies.append(copy)
    for copy in copies:
        copy.wait()


def local(lesser_in, retarded, coupling, interaction):
    order = coupling.shape[-1]
    groups = lax.axis_size("energy")
    sections = lax.axis_size("space")
    length = interaction.shape[1]
    rows = order // groups
    pieces = 2
    parts = 2 if rows % 16 == 0 else 1
    share = rows // parts
    assert lesser_in.shape[0] == 1 and coupling.shape[0] == 1
    late = list(range(1, groups, 2)) if sections > 1 and groups % 2 == 0 else []
    forward = jnp.asarray(forward_matrix(list(range(groups)) + late, length, share))
    inverse = jnp.asarray(inverse_matrix(groups, length, share))
    dma = pltpu.SemaphoreType.DMA
    matrix = (2, order, order)
    spread = (parts, groups, 2 * share, order)
    landed = pl.pallas_call(
        functools.partial(kernel, sections, groups, rows, length, pieces, parts),
        out_shape=jax.ShapeDtypeStruct((groups, parts, 2, share, order), LOW),
        in_specs=[ANY] * 6,
        out_specs=pl.BlockSpec(memory_space=pltpu.VMEM),
        scratch_shapes=[
            pltpu.VMEM(matrix, LOW),
            pltpu.VMEM(matrix, LOW),
            pltpu.VMEM(matrix, LOW),
            pltpu.VMEM(interaction.shape[1:], LOW),
            pltpu.VMEM(forward.shape, LOW),
            pltpu.VMEM(inverse.shape, LOW),
            pltpu.VMEM(matrix, WIDE),
            pltpu.VMEM(matrix, LOW),
            pltpu.VMEM(matrix, LOW),
            pltpu.VMEM(matrix, LOW),
            pltpu.VMEM(matrix, LOW),
            pltpu.VMEM(matrix, LOW),
            pltpu.VMEM(spread, LOW),
            pltpu.VMEM((parts, groups + len(late), 2 * share, order), LOW),
            pltpu.VMEM(spread, LOW),
            pltpu.VMEM((share * 2 * length, order), LOW),
            pltpu.VMEM((parts, groups, 2, share, order), LOW),
            dma((6,)),
            dma((pieces,)),
            dma((pieces,)),
            dma((pieces,)),
            dma((pieces,)),
            dma((parts, groups)),
            dma((parts, groups)),
            dma((parts, groups)),
            dma((parts, max(1, len(late)))),
            dma((parts, groups)),
            dma((parts, groups)),
            dma((2, parts)),
        ],
        compiler_params=pltpu.CompilerParams(collective_id=0, has_side_effects=True),
    )(lesser_in, retarded, coupling, interaction, forward, inverse)
    out = pl.pallas_call(
        functools.partial(write, parts),
        out_shape=jax.ShapeDtypeStruct((2, groups, parts, share, order), LOW),
        in_specs=[pl.BlockSpec(memory_space=pltpu.VMEM)],
        out_specs=ANY,
        scratch_shapes=[dma((parts, 2))],
    )(landed)
    return out.reshape(1, 1, 2, order, order)


def solution(mesh):
    in_specs = (
        P("energy", "space", None, None, None),
        P("energy", "space", None, None, None),
        P("space", None, None, None),
        P("space", None, "energy"),
    )
    out_specs = P("energy", "space", None, None, None)
    return jax.shard_map(local, mesh=mesh, in_specs=in_specs, out_specs=out_specs, check_vma=False)
```

```python
import functools
import math

import jax
import jax.numpy as jnp
import numpy as np
from jax import lax
from jax.experimental import pallas as pl
from jax.experimental.pallas import tpu as pltpu
from jax.sharding import PartitionSpec as P

MESH = pl.DeviceIdType.MESH
ANY = pl.BlockSpec(memory_space=pl.ANY)
LOW, WIDE = jnp.bfloat16, jnp.float32


def phase_parts(row_count, column_count, length):
    residue = np.arange(row_count)[:, None] * np.arange(column_count)[None, :] % length
    phase = residue * (2.0 * math.pi / length)
    return np.cos(phase), np.sin(phase)


def forward_matrix(energies, length, rows):
    cosine, sine = phase_parts(length, max(energies) + 1, length)
    cosine, sine = cosine[:, energies], sine[:, energies]
    small = np.array([[cosine, sine], [-sine, cosine]])
    full = np.einsum("pqfe,rs->rpfeqs", small, np.eye(rows))
    return full.reshape(rows * 2 * length, len(energies) * 2 * rows).astype(LOW)


def inverse_matrix(energy_count, length, rows):
    cosine, sine = phase_parts(energy_count, length, length)
    small = np.array([[cosine, -sine], [sine, cosine]])
    full = np.einsum("pqef,rs->eprsqf", small, np.eye(rows))
    return full.reshape(energy_count * 2 * rows, rows * 2 * length).astype(LOW)


def dot(left, right):
    return jnp.dot(left, right, preferred_element_type=WIDE)


def dot_t(left, right):
    return lax.dot_general(left, right, (((1,), (1,)), ((), ())), preferred_element_type=WIDE)


def product(a_re, a_im, b_re, b_im):
    return dot(a_re, b_re) + dot(-a_im, b_im), dot(a_re, b_im) + dot(a_im, b_re)


def product_adjoint(a_re, a_im, b_re, b_im):
    return dot_t(a_re, b_re) + dot_t(a_im, b_im), dot_t(a_im, b_re) + dot_t(-a_re, b_im)


def flipped(index, mask):
    bit = 1
    while bit <= mask:
        if mask & bit:
            index = index + bit - 2 * bit * (index // bit % 2)
        bit *= 2
    return index


def kernel(
    sections, groups, rows, length, pieces, parts,
    lesser_hbm, retarded_hbm, coupling_hbm, interaction_hbm, forward_hbm, inverse_hbm,
    landed,
    lesser, retarded, coupling, interaction, forward, inverse,
    total, maps, green, before, theirs, carried, homing, homed, grown, weighted, leaving,
    load_sem, hop_send, hop_recv, map_send, map_recv, go_send, go_recv, late_send, late_recv,
    back_send, back_recv, turn,
):
    section = lax.axis_index("space")
    me = lax.axis_index("energy")
    order = green.shape[-1]
    width = order // pieces
    last = sections - 1
    split = sections > 1 and groups % 2 == 0
    half = groups // 2 if split else 0
    odd = me % 2 == 1 if split else me < 0
    is_last = section == last
    feeds = (section < last - 1) | ((section == last - 1) & ~odd)
    fed = (section > 0) & ((section < last) | ~odd)
    lends = is_last & odd & (section > 0)
    grows = (section == last - 1) & odd

    if groups & (groups - 1) == 0:
        peers = [flipped(me, mask) for mask in range(groups - 1, 0, -1)]
    else:
        peers = [lax.rem(me + step, groups) for step in range(1, groups)]

    barrier = pltpu.get_barrier_semaphore()
    for peer in peers:
        pl.semaphore_signal(barrier, inc=1, device_id={"energy": peer}, device_id_type=MESH)

    @pl.when(fed)
    def _():
        pl.semaphore_signal(barrier, inc=1, device_id={"space": section - 1}, device_id_type=MESH)

    if split:
        @pl.when(grows)
        def _():
            pl.semaphore_signal(barrier, inc=1, device_id={"space": last}, device_id_type=MESH)

        @pl.when(is_last)
        def _():
            for at in range(half):
                pl.semaphore_signal(
                    barrier, inc=1,
                    device_id={"space": last - 1, "energy": 2 * at + 1}, device_id_type=MESH,
                )

    loads = []
    for at, (source, target) in enumerate((
        (retarded_hbm.at[0, 0], retarded),
        (lesser_hbm.at[0, 0], lesser),
        (coupling_hbm.at[0], coupling),
        (interaction_hbm.at[0], interaction),
        (forward_hbm, forward),
        (inverse_hbm, inverse),
    )):
        load = pltpu.make_async_copy(source, target, load_sem.at[at])
        loads.append(load)
        if target is coupling:
            pl.when(section > 0)(load.start)
        else:
            load.start()

    def arrived():
        pl.semaphore_wait(
            barrier,
            groups - 1 + jnp.where(feeds, 1, 0) + jnp.where(lends, 1, 0)
            + jnp.where(grows, groups, 0),
        )

    def hop(piece):
        columns = pl.ds(piece * width, width)
        return pltpu.make_async_remote_copy(
            src_ref=green.at[:, :, columns],
            dst_ref=before.at[:, :, columns],
            send_sem=hop_send.at[piece],
            recv_sem=hop_recv.at[piece],
            device_id={"space": section + 1},
            device_id_type=MESH,
        )

    def lend(piece):
        lines = pl.ds(piece * width, width)
        return pltpu.make_async_remote_copy(
            src_ref=maps.at[:, lines, :],
            dst_ref=theirs.at[:, lines, :],
            send_sem=map_send.at[piece],
            recv_sem=map_recv.at[piece],
            device_id={"space": section - 1},
            device_id_type=MESH,
        )

    def make_maps():
        loads[2].wait()
        m_re, m_im = product(retarded[0], retarded[1], coupling[0], coupling[1])
        maps[0], maps[1] = m_re.astype(LOW), m_im.astype(LOW)

    loads[0].wait()

    @pl.when(lends)
    def _():
        make_maps()
        arrived()
        for piece in range(pieces):
            lend(piece).start()

    loads[1].wait()
    r_re, r_im = retarded[0], retarded[1]
    half_re, half_im = product(r_re, r_im, lesser[0], lesser[1])
    half_re, half_im = half_re.astype(LOW), half_im.astype(LOW)
    total[0], total[1] = product_adjoint(half_re, half_im, r_re, r_im)

    @pl.when(~lends)
    def _():
        arrived()

    @pl.when(fed)
    def _():
        make_maps()
        for piece in range(pieces):
            hop(piece).wait_recv()
            part = slice(piece * width, (piece + 1) * width)
            k_re, k_im = product(maps[0], maps[1], before[0, :, part], before[1, :, part])
            g_re, g_im = product_adjoint(
                k_re.astype(LOW), k_im.astype(LOW), maps[0, :, part], maps[1, :, part]
            )
            total[0] += g_re
            total[1] += g_im

    @pl.when(feeds | grows)
    def _():
        green[...] = total[...].astype(LOW)

    @pl.when(feeds)
    def _():
        for piece in range(pieces):
            hop(piece).start()

    share = rows // parts

    def scattered(values, target):
        for part in range(parts):
            target[part] = jnp.concatenate(
                [values[side].reshape(groups, parts, share, order)[:, part] for side in range(2)],
                axis=1,
            ).astype(LOW).reshape(groups, 2 * share, order)

    def go(part, peer, slot):
        return pltpu.make_async_remote_copy(
            src_ref=homing.at[part, peer],
            dst_ref=homed.at[part, slot],
            send_sem=go_send,
            recv_sem=go_recv.at[part],
            device_id={"energy": peer},
            device_id_type=MESH,
        )

    def late(part, peer, slot):
        return pltpu.make_async_remote_copy(
            src_ref=grown.at[part, peer],
            dst_ref=homed.at[part, groups + slot],
            send_sem=late_send,
            recv_sem=late_recv.at[part],
            device_id={"space": last, "energy": peer},
            device_id_type=MESH,
        )

    def back(part, peer, slot):
        return pltpu.make_async_remote_copy(
            src_ref=leaving.at[part, peer],
            dst_ref=landed.at[slot, part],
            send_sem=back_send,
            recv_sem=back_recv,
            device_id={"energy": peer},
            device_id_type=MESH,
        )

    def drain(ref, sem):
        pltpu.make_async_copy(ref, ref, sem).wait()

    scattered((total[0], total[1]), homing)
    for part in range(parts):
        for peer in peers:
            go(part, peer, me).start()
        homed[part, me] = homing[part, me]

    if split:
        @pl.when(grows)
        def _():
            for piece in range(pieces):
                lend(piece).wait_recv()
                part = slice(piece * width, (piece + 1) * width)
                k_re, k_im = product(theirs[0, part, :], theirs[1, part, :], green[0], green[1])
                carried[0, part, :], carried[1, part, :] = k_re.astype(LOW), k_im.astype(LOW)
            g_re, g_im = product_adjoint(carried[0], carried[1], theirs[0], theirs[1])
            scattered((g_re, g_im), grown)
            for part in range(parts):
                for peer in peers + [me]:
                    late(part, peer, me // 2).start()

        @pl.when(~is_last)
        def _():
            for part in range(parts):
                homed[part, groups:] = jnp.zeros((half, 2 * share, order), LOW)

    for load in loads[3:]:
        load.wait()

    stride = 2 * length
    chunk = max(1, order // stride)
    for part in range(parts):
        drain(homed.at[part, :groups - 1], go_recv.at[part])
        if split:
            @pl.when(is_last)
            def _():
                drain(homed.at[part, groups:], late_recv.at[part])
        entries = homed[part]
        if 2 * share % 16:
            entries = entries.astype(WIDE)
        entries = entries.reshape((groups + half) * 2 * share, order).astype(LOW)
        for first in range(0, share, chunk):
            spectrum = dot(forward[first * stride:(first + chunk) * stride, :], entries)
            spectrum = spectrum * groups ** -0.5
            for at in range(chunk):
                row = first + at
                s_re = spectrum[at * stride:at * stride + length]
                s_im = spectrum[at * stride + length:(at + 1) * stride]
                entry = (part * share + row) * order
                weight = interaction[:, entry:entry + order].astype(WIDE)
                weighted[row * stride:row * stride + length, :] = (
                    (s_re * s_re - s_im * s_im) * weight
                ).astype(LOW)
                weighted[row * stride + length:(row + 1) * stride, :] = (
                    2.0 * s_re * s_im * weight
                ).astype(LOW)
        result = dot(inverse[...], weighted[...]) * length ** -0.5
        leaving[part] = result.reshape(groups, 2, share, order).astype(LOW)
        if split and part == 0:
            @pl.when(grows)
            def _():
                drain(grown, late_send)
                pl.semaphore_signal(turn, inc=1, device_id={"energy": me - 1}, device_id_type=MESH)

            @pl.when((section == last - 1) & ~odd)
            def _():
                pl.semaphore_wait(turn, 1)
        for peer in peers:
            back(part, peer, me).start()
        landed[me, part] = leaving[part, me]

    drain(homing.at[:, :groups - 1], go_send)

    @pl.when(feeds)
    def _():
        for piece in range(pieces):
            hop(piece).wait_send()

    if split:
        @pl.when(lends)
        def _():
            for piece in range(pieces):
                lend(piece).wait_send()

    drain(leaving.at[:, :groups - 1], back_send)
    drain(landed.at[:groups - 1], back_recv)


def local(lesser_in, retarded, coupling, interaction):
    order = coupling.shape[-1]
    groups = lax.axis_size("energy")
    sections = lax.axis_size("space")
    length = interaction.shape[1]
    rows = order // groups
    pieces = 2
    parts = 2 if rows % 16 == 0 else 1
    share = rows // parts
    assert lesser_in.shape[0] == 1 and coupling.shape[0] == 1
    late = list(range(1, groups, 2)) if sections > 1 and groups % 2 == 0 else []
    forward = jnp.asarray(forward_matrix(list(range(groups)) + late, length, share))
    inverse = jnp.asarray(inverse_matrix(groups, length, share))
    dma = pltpu.SemaphoreType.DMA
    matrix = (2, order, order)
    spread = (parts, groups, 2 * share, order)
    landed = pl.pallas_call(
        functools.partial(kernel, sections, groups, rows, length, pieces, parts),
        out_shape=pltpu.VMEM((groups, parts, 2, share, order), LOW),
        in_specs=[ANY] * 6,
        out_specs=pl.BlockSpec(memory_space=pltpu.VMEM),
        scratch_shapes=[
            pltpu.VMEM(matrix, LOW),
            pltpu.VMEM(matrix, LOW),
            pltpu.VMEM(matrix, LOW),
            pltpu.VMEM(interaction.shape[1:], LOW),
            pltpu.VMEM(forward.shape, LOW),
            pltpu.VMEM(inverse.shape, LOW),
            pltpu.VMEM(matrix, WIDE),
            pltpu.VMEM(matrix, LOW),
            pltpu.VMEM(matrix, LOW),
            pltpu.VMEM(matrix, LOW),
            pltpu.VMEM(matrix, LOW),
            pltpu.VMEM(matrix, LOW),
            pltpu.VMEM(spread, LOW),
            pltpu.VMEM((parts, groups + len(late), 2 * share, order), LOW),
            pltpu.VMEM(spread, LOW),
            pltpu.VMEM((share * 2 * length, order), LOW),
            pltpu.VMEM((parts, groups, 2, share, order), LOW),
            dma((6,)),
            dma((pieces,)),
            dma((pieces,)),
            dma((pieces,)),
            dma((pieces,)),
            dma,
            dma((parts,)),
            dma,
            dma((parts,)),
            dma,
            dma,
            pltpu.SemaphoreType.REGULAR,
        ],
        compiler_params=pltpu.CompilerParams(collective_id=0, has_side_effects=True),
    )(lesser_in, retarded, coupling, interaction, forward, inverse)
    out = landed.transpose(2, 0, 1, 3, 4)
    return out.reshape(1, 1, 2, order, order)


def solution(mesh):
    in_specs = (
        P("energy", "space", None, None, None),
        P("energy", "space", None, None, None),
        P("space", None, None, None),
        P("space", None, "energy"),
    )
    out_specs = P("energy", "space", None, None, None)
    return jax.shard_map(local, mesh=mesh, in_specs=in_specs, out_specs=out_specs, check_vma=False)
```

```python
import functools
import math

import jax
import jax.numpy as jnp
import numpy as np
from jax import lax
from jax.experimental import pallas as pl
from jax.experimental.pallas import tpu as pltpu
from jax.sharding import PartitionSpec as P

MESH = pl.DeviceIdType.MESH
ANY = pl.BlockSpec(memory_space=pl.ANY)
LOW, WIDE = jnp.bfloat16, jnp.float32


def phase_parts(row_count, column_count, length):
    residue = np.arange(row_count)[:, None] * np.arange(column_count)[None, :] % length
    phase = residue * (2.0 * math.pi / length)
    return np.cos(phase), np.sin(phase)


def forward_matrix(energies, length, rows):
    cosine, sine = phase_parts(length, max(energies) + 1, length)
    cosine, sine = cosine[:, energies], sine[:, energies]
    small = np.array([[cosine, sine], [-sine, cosine]])
    full = np.einsum("pqfe,rs->rpfeqs", small, np.eye(rows))
    return full.reshape(rows * 2 * length, len(energies) * 2 * rows).astype(LOW)


def inverse_matrix(energy_count, length, rows):
    cosine, sine = phase_parts(energy_count, length, length)
    small = np.array([[cosine, -sine], [sine, cosine]])
    full = np.einsum("pqef,rs->eprsqf", small, np.eye(rows))
    return full.reshape(energy_count * 2 * rows, rows * 2 * length).astype(LOW)


def dot(left, right):
    return jnp.dot(left, right, preferred_element_type=WIDE)


def dot_t(left, right):
    return lax.dot_general(left, right, (((1,), (1,)), ((), ())), preferred_element_type=WIDE)


def product(a_re, a_im, b_re, b_im):
    return dot(a_re, b_re) + dot(-a_im, b_im), dot(a_re, b_im) + dot(a_im, b_re)


def product_adjoint(a_re, a_im, b_re, b_im):
    return dot_t(a_re, b_re) + dot_t(a_im, b_im), dot_t(a_im, b_re) + dot_t(-a_re, b_im)


def flipped(index, mask):
    bit = 1
    while bit <= mask:
        if mask & bit:
            index = index + bit - 2 * bit * (index // bit % 2)
        bit *= 2
    return index


def kernel(
    sections, groups, rows, length, pieces, parts,
    lesser_hbm, retarded_hbm, coupling_hbm, interaction_hbm, forward_hbm, inverse_hbm,
    landed,
    lesser, retarded, coupling, interaction, forward, inverse,
    total, maps, green, before, theirs, carried, homing, homed, grown, weighted, leaving,
    load_sem, hop_send, hop_recv, map_send, map_recv, go_send, go_recv, late_send, late_recv,
    back_send, back_recv, turn, ready, clear,
):
    section = lax.axis_index("space")
    me = lax.axis_index("energy")
    order = green.shape[-1]
    width = order // pieces
    last = sections - 1
    split = sections > 1 and groups % 2 == 0
    half = groups // 2 if split else 0
    odd = me % 2 == 1 if split else me < 0
    is_last = section == last
    feeds = (section < last - 1) | ((section == last - 1) & ~odd)
    fed = (section > 0) & ((section < last) | ~odd)
    lends = is_last & odd & (section > 0)
    grows = (section == last - 1) & odd

    if groups & (groups - 1) == 0:
        peers = [flipped(me, mask) for mask in range(groups - 1, 0, -1)]
    else:
        peers = [lax.rem(me + step, groups) for step in range(1, groups)]

    collects = (me + section // max(last, 1)) % 2 == 1 if split else me >= 0
    barrier = pltpu.get_barrier_semaphore()
    if split:
        for at in range(half):
            peer = 2 * at + 1 - section // last

            @pl.when(peer != me)
            def _():
                pl.semaphore_signal(
                    barrier, inc=1, device_id={"energy": peer}, device_id_type=MESH
                )

        @pl.when(grows)
        def _():
            pl.semaphore_signal(barrier, inc=1, device_id={"space": last}, device_id_type=MESH)
    else:
        for peer in peers:
            pl.semaphore_signal(barrier, inc=1, device_id={"energy": peer}, device_id_type=MESH)

    @pl.when(fed)
    def _():
        pl.semaphore_signal(barrier, inc=1, device_id={"space": section - 1}, device_id_type=MESH)

    loads = []
    for at, (source, target) in enumerate((
        (retarded_hbm.at[0, 0], retarded),
        (lesser_hbm.at[0, 0], lesser),
        (coupling_hbm.at[0], coupling),
        (interaction_hbm.at[0], interaction),
        (forward_hbm, forward),
        (inverse_hbm, inverse),
    )):
        load = pltpu.make_async_copy(source, target, load_sem.at[at])
        loads.append(load)
        if target is coupling:
            pl.when(section > 0)(load.start)
        else:
            load.start()

    def across():
        @pl.when(~collects)
        def _():
            pl.semaphore_wait(barrier, 1)

    def gathered():
        @pl.when(collects)
        def _():
            pl.semaphore_wait(barrier, groups - 1 + jnp.where(feeds, 1, 0))
            if split:
                pl.semaphore_signal(
                    ready, inc=1,
                    device_id={"energy": me + 1 - 2 * (me % 2)}, device_id_type=MESH,
                )

    def told():
        @pl.when(~collects)
        def _():
            pl.semaphore_wait(ready, 1)

        @pl.when(lends)
        def _():
            pl.semaphore_signal(clear, inc=1, device_id={"space": last - 1}, device_id_type=MESH)

    def hop(piece):
        columns = pl.ds(piece * width, width)
        return pltpu.make_async_remote_copy(
            src_ref=green.at[:, :, columns],
            dst_ref=before.at[:, :, columns],
            send_sem=hop_send.at[piece],
            recv_sem=hop_recv.at[piece],
            device_id={"space": section + 1},
            device_id_type=MESH,
        )

    def lend(piece):
        lines = pl.ds(piece * width, width)
        return pltpu.make_async_remote_copy(
            src_ref=maps.at[:, lines, :],
            dst_ref=theirs.at[:, lines, :],
            send_sem=map_send.at[piece],
            recv_sem=map_recv.at[piece],
            device_id={"space": section - 1},
            device_id_type=MESH,
        )

    def make_maps():
        loads[2].wait()
        m_re, m_im = product(retarded[0], retarded[1], coupling[0], coupling[1])
        maps[0], maps[1] = m_re.astype(LOW), m_im.astype(LOW)

    loads[0].wait()

    @pl.when(lends)
    def _():
        make_maps()
        across()
        for piece in range(pieces):
            lend(piece).start()

    loads[1].wait()
    r_re, r_im = retarded[0], retarded[1]
    half_re, half_im = product(r_re, r_im, lesser[0], lesser[1])
    half_re, half_im = half_re.astype(LOW), half_im.astype(LOW)
    total[0], total[1] = product_adjoint(half_re, half_im, r_re, r_im)

    @pl.when(~lends)
    def _():
        across()
        gathered()

    @pl.when(fed)
    def _():
        make_maps()
        for piece in range(pieces):
            hop(piece).wait_recv()
            part = slice(piece * width, (piece + 1) * width)
            k_re, k_im = product(maps[0], maps[1], before[0, :, part], before[1, :, part])
            g_re, g_im = product_adjoint(
                k_re.astype(LOW), k_im.astype(LOW), maps[0, :, part], maps[1, :, part]
            )
            total[0] += g_re
            total[1] += g_im

    @pl.when(feeds | grows)
    def _():
        green[...] = total[...].astype(LOW)

    @pl.when(feeds)
    def _():
        for piece in range(pieces):
            hop(piece).start()

    share = rows // parts

    def scattered(values, target):
        for part in range(parts):
            target[part] = jnp.concatenate(
                [values[side].reshape(groups, parts, share, order)[:, part] for side in range(2)],
                axis=1,
            ).astype(LOW).reshape(groups, 2 * share, order)

    def go(part, peer, slot):
        return pltpu.make_async_remote_copy(
            src_ref=homing.at[part, peer],
            dst_ref=homed.at[part, slot],
            send_sem=go_send,
            recv_sem=go_recv.at[part],
            device_id={"energy": peer},
            device_id_type=MESH,
        )

    def late(part, peer, slot):
        return pltpu.make_async_remote_copy(
            src_ref=grown.at[part, peer],
            dst_ref=homed.at[part, groups + slot],
            send_sem=late_send,
            recv_sem=late_recv.at[part],
            device_id={"space": last, "energy": peer},
            device_id_type=MESH,
        )

    def back(part, peer, slot):
        return pltpu.make_async_remote_copy(
            src_ref=leaving.at[part, peer],
            dst_ref=landed.at[slot, part],
            send_sem=back_send,
            recv_sem=back_recv,
            device_id={"energy": peer},
            device_id_type=MESH,
        )

    def drain(ref, sem):
        pltpu.make_async_copy(ref, ref, sem).wait()

    scattered((total[0], total[1]), homing)
    if split:
        told()
    for part in range(parts):
        for peer in peers:
            go(part, peer, me).start()
        homed[part, me] = homing[part, me]

    if split:
        @pl.when(grows)
        def _():
            for piece in range(pieces):
                lend(piece).wait_recv()
                part = slice(piece * width, (piece + 1) * width)
                k_re, k_im = product(theirs[0, part, :], theirs[1, part, :], green[0], green[1])
                carried[0, part, :], carried[1, part, :] = k_re.astype(LOW), k_im.astype(LOW)
            g_re, g_im = product_adjoint(carried[0], carried[1], theirs[0], theirs[1])
            scattered((g_re, g_im), grown)
            pl.semaphore_wait(clear, 1)
            for part in range(parts):
                for peer in peers + [me]:
                    late(part, peer, me // 2).start()

        @pl.when(~is_last)
        def _():
            for part in range(parts):
                homed[part, groups:] = jnp.zeros((half, 2 * share, order), LOW)

    for load in loads[3:]:
        load.wait()

    stride = 2 * length
    chunk = max(1, order // stride)
    for part in range(parts):
        drain(homed.at[part, :groups - 1], go_recv.at[part])
        if split:
            @pl.when(is_last)
            def _():
                drain(homed.at[part, groups:], late_recv.at[part])
        entries = homed[part]
        if 2 * share % 16:
            entries = entries.astype(WIDE)
        entries = entries.reshape((groups + half) * 2 * share, order).astype(LOW)
        for first in range(0, share, chunk):
            spectrum = dot(forward[first * stride:(first + chunk) * stride, :], entries)
            spectrum = spectrum * groups ** -0.5
            for at in range(chunk):
                row = first + at
                s_re = spectrum[at * stride:at * stride + length]
                s_im = spectrum[at * stride + length:(at + 1) * stride]
                entry = (part * share + row) * order
                weight = interaction[:, entry:entry + order].astype(WIDE)
                weighted[row * stride:row * stride + length, :] = (
                    (s_re * s_re - s_im * s_im) * weight
                ).astype(LOW)
                weighted[row * stride + length:(row + 1) * stride, :] = (
                    2.0 * s_re * s_im * weight
                ).astype(LOW)
        result = dot(inverse[...], weighted[...]) * length ** -0.5
        leaving[part] = result.reshape(groups, 2, share, order).astype(LOW)
        if split and part == 0:
            @pl.when(grows)
            def _():
                drain(grown, late_send)
                pl.semaphore_signal(turn, inc=1, device_id={"energy": me - 1}, device_id_type=MESH)

            @pl.when((section == last - 1) & ~odd)
            def _():
                pl.semaphore_wait(turn, 1)
        for peer in peers:
            back(part, peer, me).start()
        landed[me, part] = leaving[part, me]

    drain(homing.at[:, :groups - 1], go_send)

    @pl.when(feeds)
    def _():
        for piece in range(pieces):
            hop(piece).wait_send()

    if split:
        @pl.when(lends)
        def _():
            for piece in range(pieces):
                lend(piece).wait_send()

    drain(leaving.at[:, :groups - 1], back_send)
    drain(landed.at[:groups - 1], back_recv)


def local(lesser_in, retarded, coupling, interaction):
    order = coupling.shape[-1]
    groups = lax.axis_size("energy")
    sections = lax.axis_size("space")
    length = interaction.shape[1]
    rows = order // groups
    pieces = 2
    parts = 2 if rows % 16 == 0 else 1
    share = rows // parts
    assert lesser_in.shape[0] == 1 and coupling.shape[0] == 1
    late = list(range(1, groups, 2)) if sections > 1 and groups % 2 == 0 else []
    forward = jnp.asarray(forward_matrix(list(range(groups)) + late, length, share))
    inverse = jnp.asarray(inverse_matrix(groups, length, share))
    dma = pltpu.SemaphoreType.DMA
    matrix = (2, order, order)
    spread = (parts, groups, 2 * share, order)
    landed = pl.pallas_call(
        functools.partial(kernel, sections, groups, rows, length, pieces, parts),
        out_shape=pltpu.VMEM((groups, parts, 2, share, order), LOW),
        in_specs=[ANY] * 6,
        out_specs=pl.BlockSpec(memory_space=pltpu.VMEM),
        scratch_shapes=[
            pltpu.VMEM(matrix, LOW),
            pltpu.VMEM(matrix, LOW),
            pltpu.VMEM(matrix, LOW),
            pltpu.VMEM(interaction.shape[1:], LOW),
            pltpu.VMEM(forward.shape, LOW),
            pltpu.VMEM(inverse.shape, LOW),
            pltpu.VMEM(matrix, WIDE),
            pltpu.VMEM(matrix, LOW),
            pltpu.VMEM(matrix, LOW),
            pltpu.VMEM(matrix, LOW),
            pltpu.VMEM(matrix, LOW),
            pltpu.VMEM(matrix, LOW),
            pltpu.VMEM(spread, LOW),
            pltpu.VMEM((parts, groups + len(late), 2 * share, order), LOW),
            pltpu.VMEM(spread, LOW),
            pltpu.VMEM((share * 2 * length, order), LOW),
            pltpu.VMEM((parts, groups, 2, share, order), LOW),
            dma((6,)),
            dma((pieces,)),
            dma((pieces,)),
            dma((pieces,)),
            dma((pieces,)),
            dma,
            dma((parts,)),
            dma,
            dma((parts,)),
            dma,
            dma,
            pltpu.SemaphoreType.REGULAR,
            pltpu.SemaphoreType.REGULAR,
            pltpu.SemaphoreType.REGULAR,
        ],
        compiler_params=pltpu.CompilerParams(collective_id=0, has_side_effects=True),
    )(lesser_in, retarded, coupling, interaction, forward, inverse)
    out = landed.transpose(2, 0, 1, 3, 4)
    return out.reshape(1, 1, 2, order, order)


def solution(mesh):
    in_specs = (
        P("energy", "space", None, None, None),
        P("energy", "space", None, None, None),
        P("space", None, None, None),
        P("space", None, "energy"),
    )
    out_specs = P("energy", "space", None, None, None)
    return jax.shard_map(local, mesh=mesh, in_specs=in_specs, out_specs=out_specs, check_vma=False)
```

```python
import functools
import math

import jax
import jax.numpy as jnp
import numpy as np
from jax import lax
from jax.experimental import pallas as pl
from jax.experimental.pallas import tpu as pltpu
from jax.sharding import PartitionSpec as P

MESH = pl.DeviceIdType.MESH
ANY = pl.BlockSpec(memory_space=pl.ANY)
LOW, WIDE = jnp.bfloat16, jnp.float32


def phase_parts(row_count, column_count, length):
    residue = np.arange(row_count)[:, None] * np.arange(column_count)[None, :] % length
    phase = residue * (2.0 * math.pi / length)
    return np.cos(phase), np.sin(phase)


def forward_matrix(energies, length, rows):
    cosine, sine = phase_parts(length, max(energies) + 1, length)
    cosine, sine = cosine[:, energies], sine[:, energies]
    small = np.array([[cosine, sine], [-sine, cosine]])
    full = np.einsum("pqfe,rs->rpfeqs", small, np.eye(rows))
    return full.reshape(rows * 2 * length, len(energies) * 2 * rows).astype(LOW)


def inverse_matrix(energy_count, length, rows):
    cosine, sine = phase_parts(energy_count, length, length)
    small = np.array([[cosine, -sine], [sine, cosine]])
    full = np.einsum("pqef,rs->eprsqf", small, np.eye(rows))
    return full.reshape(energy_count * 2 * rows, rows * 2 * length).astype(LOW)


def dot(left, right):
    return jnp.dot(left, right, preferred_element_type=WIDE)


def dot_t(left, right):
    return lax.dot_general(left, right, (((1,), (1,)), ((), ())), preferred_element_type=WIDE)


def product(a_re, a_im, b_re, b_im):
    return dot(a_re, b_re) + dot(-a_im, b_im), dot(a_re, b_im) + dot(a_im, b_re)


def product_adjoint(a_re, a_im, b_re, b_im):
    return dot_t(a_re, b_re) + dot_t(a_im, b_im), dot_t(a_im, b_re) + dot_t(-a_re, b_im)


def beside(first, second, axis):
    return jnp.concatenate([first, second], axis=axis)


def flipped(index, mask):
    bit = 1
    while bit <= mask:
        if mask & bit:
            index = index + bit - 2 * bit * (index // bit % 2)
        bit *= 2
    return index


def kernel(
    sections, groups, rows, length, pieces, parts,
    lesser_hbm, retarded_hbm, coupling_hbm, interaction_hbm, forward_hbm, inverse_hbm,
    landed,
    lesser, retarded, coupling, interaction, forward, inverse,
    total, maps, green, before, theirs, carried, homing, homed, grown, repaid, weighted, leaving, passing,
    load_sem, hop_send, hop_recv, map_send, map_recv, go_send, go_recv, late_send, late_recv,
    pay_send, pay_recv, back_send, back_recv, relay_send, relay_recv, pass_send, turn, ready, clear,
):
    section = lax.axis_index("space")
    me = lax.axis_index("energy")
    order = green.shape[-1]
    width = order // pieces
    last = sections - 1
    split = sections > 1 and groups % 2 == 0
    half = groups // 2 if split else 0
    direct = parts - parts // 4
    relays = split and groups % 4 == 0 and groups & (groups - 1) == 0
    quarter = groups // 4 if relays else 0
    odd = me % 2 == 1 if split else me < 0
    is_last = section == last
    feeds = (section < last - 1) | ((section == last - 1) & ~odd)
    fed = (section > 0) & ((section < last) | ~odd)
    lends = is_last & odd & (section > 0)
    grows = (section == last - 1) & odd

    if groups & (groups - 1) == 0:
        peers = [flipped(me, mask) for mask in range(groups - 1, 0, -1)]
    else:
        peers = [lax.rem(me + step, groups) for step in range(1, groups)]
    homeward, mirrored = peers, 0
    if relays:
        own, low = me // quarter, me % quarter
        over = 2 * (1 - own // 2)
        mirrored = (over + 1) * quarter
        homeward = [
            to * quarter + flipped(low, mask)
            for to in (over + 1, over, own + 1 - 2 * (own % 2), own)
            for mask in range(quarter - 1, -1, -1)
        ][:-1]

    loads = []
    for at, (source, target) in enumerate((
        (retarded_hbm.at[0, 0], retarded),
        (lesser_hbm.at[0, 0], lesser),
        (coupling_hbm.at[0], coupling),
        (interaction_hbm.at[0], interaction),
        (forward_hbm, forward),
        (inverse_hbm, inverse),
    )):
        load = pltpu.make_async_copy(source, target, load_sem.at[at])
        loads.append(load)
        if target is coupling:
            pl.when(section > 0)(load.start)
        elif at < 2:
            load.start()

    collects = (me + section // max(last, 1)) % 2 == 1 if split else me >= 0
    barrier = pltpu.get_barrier_semaphore()
    if split:
        for at in range(half):
            peer = 2 * at + 1 - section // last

            @pl.when(peer != me)
            def _():
                pl.semaphore_signal(
                    barrier, inc=1, device_id={"energy": peer}, device_id_type=MESH
                )

        @pl.when(grows)
        def _():
            pl.semaphore_signal(barrier, inc=1, device_id={"space": last}, device_id_type=MESH)
    else:
        for peer in peers:
            pl.semaphore_signal(barrier, inc=1, device_id={"energy": peer}, device_id_type=MESH)

    @pl.when(fed)
    def _():
        pl.semaphore_signal(barrier, inc=1, device_id={"space": section - 1}, device_id_type=MESH)

    def across():
        @pl.when(~collects)
        def _():
            pl.semaphore_wait(barrier, 1)

    def gathered():
        @pl.when(collects)
        def _():
            pl.semaphore_wait(barrier, groups - 1 + jnp.where(feeds, 1, 0))
            if split:
                pl.semaphore_signal(
                    ready, inc=1,
                    device_id={"energy": me + 1 - 2 * (me % 2)}, device_id_type=MESH,
                )

    def told():
        @pl.when(~collects)
        def _():
            pl.semaphore_wait(ready, 1)

        @pl.when(lends)
        def _():
            pl.semaphore_signal(clear, inc=1, device_id={"space": last - 1}, device_id_type=MESH)

    def hop(piece):
        columns = pl.ds(piece * width, width)
        return pltpu.make_async_remote_copy(
            src_ref=green.at[:, :, columns],
            dst_ref=before.at[:, :, columns],
            send_sem=hop_send.at[piece],
            recv_sem=hop_recv.at[piece],
            device_id={"space": section + 1},
            device_id_type=MESH,
        )

    def lend(piece):
        lines = pl.ds(piece * width, width)
        return pltpu.make_async_remote_copy(
            src_ref=maps.at[:, lines, :],
            dst_ref=theirs.at[:, lines, :],
            send_sem=map_send.at[piece],
            recv_sem=map_recv.at[piece],
            device_id={"space": section - 1},
            device_id_type=MESH,
        )

    def make_maps():
        loads[2].wait()
        m_re, m_im = product(retarded[0], retarded[1], coupling[0], coupling[1])
        maps[0], maps[1] = m_re.astype(LOW), m_im.astype(LOW)

    loads[0].wait()

    @pl.when(lends)
    def _():
        make_maps()
        across()
        for piece in range(pieces):
            lend(piece).start()

    loads[1].wait()
    for load in loads[3:]:
        load.start()
    r_re, r_im = retarded[0], retarded[1]
    half_re, half_im = product(r_re, r_im, lesser[0], lesser[1])
    half_re, half_im = half_re.astype(LOW), half_im.astype(LOW)
    total[0], total[1] = product_adjoint(half_re, half_im, r_re, r_im)

    @pl.when(~lends)
    def _():
        across()
        gathered()

    @pl.when(fed)
    def _():
        make_maps()
        for piece in range(pieces):
            hop(piece).wait_recv()
            part = slice(piece * width, (piece + 1) * width)
            k_re, k_im = product(maps[0], maps[1], before[0, :, part], before[1, :, part])
            g_re, g_im = product_adjoint(
                k_re.astype(LOW), k_im.astype(LOW), maps[0, :, part], maps[1, :, part]
            )
            total[0] += g_re
            total[1] += g_im

    @pl.when(feeds | grows)
    def _():
        green[...] = total[...].astype(LOW)

    @pl.when(feeds)
    def _():
        for piece in range(pieces):
            hop(piece).start()

    share = rows // parts

    def entries_of(values, part):
        sides = [
            values[side].reshape(groups, parts, share, order)[:, part] for side in range(2)
        ]
        return beside(*sides, 1)

    def scattered(values, target):
        for part in range(parts):
            target[part] = entries_of(values, part).astype(LOW)

    def go(part, peer, slot):
        return pltpu.make_async_remote_copy(
            src_ref=homing.at[part, peer],
            dst_ref=homed.at[part, slot],
            send_sem=go_send,
            recv_sem=go_recv.at[part],
            device_id={"energy": peer},
            device_id_type=MESH,
        )

    def late(part, peer, slot):
        return pltpu.make_async_remote_copy(
            src_ref=grown.at[part, peer],
            dst_ref=homed.at[part, groups + slot],
            send_sem=late_send,
            recv_sem=late_recv.at[part],
            device_id={"space": last, "energy": peer},
            device_id_type=MESH,
        )

    def pay():
        return pltpu.make_async_remote_copy(
            src_ref=grown.at[direct:],
            dst_ref=repaid,
            send_sem=pay_send,
            recv_sem=pay_recv,
            device_id={"space": last},
            device_id_type=MESH,
        )

    def back(part, peer, slot):
        return pltpu.make_async_remote_copy(
            src_ref=leaving.at[part * groups + peer],
            dst_ref=landed.at[:, slot, part],
            send_sem=back_send,
            recv_sem=back_recv,
            device_id={"energy": peer},
            device_id_type=MESH,
        )

    def drain(ref, sem):
        pltpu.make_async_copy(ref, ref, sem).wait()

    def relay():
        return pltpu.make_async_remote_copy(
            src_ref=leaving.at[pl.ds(mirrored, max(1, quarter))],
            dst_ref=passing,
            send_sem=relay_send,
            recv_sem=relay_recv,
            device_id={"space": last - 1},
            device_id_type=MESH,
        )

    def forward_on(at):
        return pltpu.make_async_remote_copy(
            src_ref=passing.at[at],
            dst_ref=landed.at[:, me, 0],
            send_sem=pass_send,
            recv_sem=back_recv,
            device_id={"space": last, "energy": mirrored + at},
            device_id_type=MESH,
        )

    scattered((total[0], total[1]), homing)
    if split:
        told()

    def send(part):
        for peer in homeward:
            go(part, peer, me).start()
        homed[part, me] = homing[part, me]

    for part in range(parts):
        if split and part >= direct:
            pl.when(~lends)(functools.partial(send, part))
        else:
            send(part)

    if split:
        @pl.when(grows)
        def _():
            for piece in range(pieces):
                lend(piece).wait_recv()
                part = slice(piece * width, (piece + 1) * width)
                k_re, k_im = product(theirs[0, part, :], theirs[1, part, :], green[0], green[1])
                carried[0, part, :], carried[1, part, :] = k_re.astype(LOW), k_im.astype(LOW)
            g_re, g_im = product_adjoint(carried[0], carried[1], theirs[0], theirs[1])
            scattered((g_re, g_im), grown)
            pl.semaphore_wait(clear, 1)
            if direct < parts:
                pay().start()
            for part in range(direct):
                for peer in peers + [me]:
                    late(part, peer, me // 2).start()

        @pl.when(~is_last)
        def _():
            for part in range(direct):
                homed[part, groups:] = jnp.zeros((half, 2 * share, order), LOW)

        if direct < parts:
            @pl.when(lends)
            def _():
                pay().wait_recv()
                for part in range(direct, parts):
                    homing[part] = (
                        entries_of((total[0], total[1]), part)
                        + repaid[part - direct].astype(WIDE)
                    ).astype(LOW)
                    send(part)

    for load in loads[3:]:
        load.wait()

    stride = 2 * length
    chunk = max(1, order // stride)
    for part in range(parts):
        drain(homed.at[part, :groups - 1], go_recv.at[part])
        if split and part < direct:
            @pl.when(is_last)
            def _():
                drain(homed.at[part, groups:], late_recv.at[part])
        count = groups + half if part < direct else groups
        entries = homed[part, :count]
        if 2 * share % 16:
            entries = entries.astype(WIDE)
        entries = entries.reshape(count * 2 * share, order).astype(LOW)
        for first in range(0, share, chunk):
            spectrum = dot(
                forward[first * stride:(first + chunk) * stride, :count * 2 * share], entries
            )
            spectrum = spectrum * groups ** -0.5
            for at in range(chunk):
                row = first + at
                s_re = spectrum[at * stride:at * stride + length]
                s_im = spectrum[at * stride + length:(at + 1) * stride]
                entry = (part * share + row) * order
                weight = interaction[:, entry:entry + order].astype(WIDE)
                weighted[row * stride:row * stride + length, :] = (
                    (s_re * s_re - s_im * s_im) * weight
                ).astype(LOW)
                weighted[row * stride + length:(row + 1) * stride, :] = (
                    2.0 * s_re * s_im * weight
                ).astype(LOW)
        result = dot(inverse[...], weighted[...]) * length ** -0.5
        leaving[part * groups:(part + 1) * groups] = (
            result.reshape(groups, 2, share, order).astype(LOW)
        )
        if split and part == 0:
            @pl.when(grows)
            def _():
                drain(grown.at[:direct], late_send)
                pl.semaphore_signal(turn, inc=1, device_id={"energy": me - 1}, device_id_type=MESH)

            @pl.when((section == last - 1) & ~odd)
            def _():
                pl.semaphore_wait(turn, 1)
        here = homeward
        if relays:
            here = homeward[quarter:2 * quarter] + homeward[2 * quarter:]
            if part == 0:
                @pl.when(is_last)
                def _():
                    relay().start()

                @pl.when(~is_last)
                def _():
                    for peer in homeward[:quarter]:
                        back(part, peer, me).start()
            else:
                here = here[:quarter] + homeward[:quarter] + here[quarter:]
        for peer in here:
            back(part, peer, me).start()
        landed[:, me, part] = leaving[part * groups + me]

    if relays:
        @pl.when(section == last - 1)
        def _():
            relay().wait_recv()
            for at in range(quarter):
                forward_on(at).start()

    drain(homing.at[:, :groups - 1], go_send)

    @pl.when(feeds)
    def _():
        for piece in range(pieces):
            hop(piece).wait_send()

    if split:
        @pl.when(lends)
        def _():
            for piece in range(pieces):
                lend(piece).wait_send()

        if direct < parts:
            @pl.when(grows)
            def _():
                pay().wait_send()

    if relays:
        @pl.when(section == last - 1)
        def _():
            drain(passing, pass_send)

        @pl.when(is_last)
        def _():
            relay().wait_send()
            drain(leaving.at[:parts * (groups - 1) - quarter], back_send)

        @pl.when(~is_last)
        def _():
            drain(leaving.at[:parts * (groups - 1)], back_send)
    else:
        drain(leaving.at[:parts * (groups - 1)], back_send)
    drain(landed.at[:, :groups - 1], back_recv)


def local(lesser_in, retarded, coupling, interaction):
    order = coupling.shape[-1]
    groups = lax.axis_size("energy")
    sections = lax.axis_size("space")
    length = interaction.shape[1]
    rows = order // groups
    pieces = 2
    parts = 4 if rows % 16 == 0 else 1
    share = rows // parts
    assert lesser_in.shape[0] == 1 and coupling.shape[0] == 1
    late = list(range(1, groups, 2)) if sections > 1 and groups % 2 == 0 else []
    forward = jnp.asarray(forward_matrix(list(range(groups)) + late, length, share))
    inverse = jnp.asarray(inverse_matrix(groups, length, share))
    dma = pltpu.SemaphoreType.DMA
    matrix = (2, order, order)
    spread = (parts, groups, 2 * share, order)
    landed = pl.pallas_call(
        functools.partial(kernel, sections, groups, rows, length, pieces, parts),
        out_shape=pltpu.VMEM((2, groups, parts, share, order), LOW),
        in_specs=[ANY] * 6,
        out_specs=pl.BlockSpec(memory_space=pltpu.VMEM),
        scratch_shapes=[
            pltpu.VMEM(matrix, LOW),
            pltpu.VMEM(matrix, LOW),
            pltpu.VMEM(matrix, LOW),
            pltpu.VMEM(interaction.shape[1:], LOW),
            pltpu.VMEM(forward.shape, LOW),
            pltpu.VMEM(inverse.shape, LOW),
            pltpu.VMEM(matrix, WIDE),
            pltpu.VMEM(matrix, LOW),
            pltpu.VMEM(matrix, LOW),
            pltpu.VMEM(matrix, LOW),
            pltpu.VMEM(matrix, LOW),
            pltpu.VMEM(matrix, LOW),
            pltpu.VMEM(spread, LOW),
            pltpu.VMEM((parts, groups + len(late), 2 * share, order), LOW),
            pltpu.VMEM(spread, LOW),
            pltpu.VMEM((max(1, parts // 4), groups, 2 * share, order), LOW),
            pltpu.VMEM((share * 2 * length, order), LOW),
            pltpu.VMEM((parts * groups, 2, share, order), LOW),
            pltpu.VMEM((max(1, groups // 4), 2, share, order), LOW),
            dma((6,)),
            dma((pieces,)),
            dma((pieces,)),
            dma((pieces,)),
            dma((pieces,)),
            dma,
            dma((parts,)),
            dma,
            dma((parts,)),
            dma,
            dma,
            dma,
            dma,
            dma,
            dma,
            dma,
            pltpu.SemaphoreType.REGULAR,
            pltpu.SemaphoreType.REGULAR,
            pltpu.SemaphoreType.REGULAR,
        ],
        compiler_params=pltpu.CompilerParams(collective_id=0, has_side_effects=True),
    )(lesser_in, retarded, coupling, interaction, forward, inverse)
    return landed.reshape(1, 1, 2, order, order)


def solution(mesh):
    in_specs = (
        P("energy", "space", None, None, None),
        P("energy", "space", None, None, None),
        P("space", None, None, None),
        P("space", None, "energy"),
    )
    out_specs = P("energy", "space", None, None, None)
    return jax.shard_map(local, mesh=mesh, in_specs=in_specs, out_specs=out_specs, check_vma=False)
```

```python
import functools
import math

import jax
import jax.numpy as jnp
import numpy as np
from jax import lax
from jax.experimental import pallas as pl
from jax.experimental.pallas import tpu as pltpu
from jax.sharding import PartitionSpec as P

MESH = pl.DeviceIdType.MESH
ANY = pl.BlockSpec(memory_space=pl.ANY)
LOW, WIDE = jnp.bfloat16, jnp.float32


def phase_parts(row_count, column_count, length):
    residue = np.arange(row_count)[:, None] * np.arange(column_count)[None, :] % length
    phase = residue * (2.0 * math.pi / length)
    return np.cos(phase), np.sin(phase)


def forward_matrix(energies, length, rows):
    cosine, sine = phase_parts(length, max(energies) + 1, length)
    cosine, sine = cosine[:, energies], sine[:, energies]
    small = np.array([[cosine, sine], [-sine, cosine]])
    full = np.einsum("pqfe,rs->rpfeqs", small, np.eye(rows))
    return full.reshape(rows * 2 * length, len(energies) * 2 * rows).astype(LOW)


def inverse_matrix(energy_count, length, rows):
    cosine, sine = phase_parts(energy_count, length, length)
    small = np.array([[cosine, -sine], [sine, cosine]])
    full = np.einsum("pqef,rs->eprsqf", small, np.eye(rows))
    return full.reshape(energy_count * 2 * rows, rows * 2 * length).astype(LOW)


def dot(left, right):
    return jnp.dot(left, right, preferred_element_type=WIDE)


def dot_t(left, right):
    return lax.dot_general(left, right, (((1,), (1,)), ((), ())), preferred_element_type=WIDE)


def product(a_re, a_im, b_re, b_im):
    return dot(a_re, b_re) + dot(-a_im, b_im), dot(a_re, b_im) + dot(a_im, b_re)


def product_adjoint(a_re, a_im, b_re, b_im):
    return dot_t(a_re, b_re) + dot_t(a_im, b_im), dot_t(a_im, b_re) + dot_t(-a_re, b_im)


def beside(first, second, axis):
    return jnp.concatenate([first, second], axis=axis)


def flipped(index, mask):
    bit = 1
    while bit <= mask:
        if mask & bit:
            index = index + bit - 2 * bit * (index // bit % 2)
        bit *= 2
    return index


def kernel(
    sections, groups, rows, length, pieces, parts,
    lesser_hbm, retarded_hbm, coupling_hbm, interaction_hbm, forward_hbm, inverse_hbm,
    landed,
    lesser, retarded, coupling, interaction, forward, inverse,
    total, maps, green, before, theirs, carried, homing, homed, grown, repaid, weighted, leaving, passing,
    load_sem, hop_send, hop_recv, map_send, map_recv, go_send, go_recv, late_send, late_recv,
    pay_send, pay_recv, back_send, back_recv, relay_send, relay_recv, pass_send, turn, ready, clear,
):
    section = lax.axis_index("space")
    me = lax.axis_index("energy")
    order = green.shape[-1]
    width = order // pieces
    last = sections - 1
    split = sections > 1 and groups % 2 == 0
    half = groups // 2 if split else 0
    direct = parts - parts // 4
    relays = split and groups % 4 == 0 and groups & (groups - 1) == 0
    quarter = groups // 4 if relays else 0
    odd = me % 2 == 1 if split else me < 0
    is_last = section == last
    feeds = (section < last - 1) | ((section == last - 1) & ~odd)
    fed = (section > 0) & ((section < last) | ~odd)
    lends = is_last & odd & (section > 0)
    grows = (section == last - 1) & odd

    if groups & (groups - 1) == 0:
        peers = [flipped(me, mask) for mask in range(groups - 1, 0, -1)]
    else:
        peers = [lax.rem(me + step, groups) for step in range(1, groups)]
    homeward, mirrored = peers, 0
    if relays:
        own, low = me // quarter, me % quarter
        over = 2 * (1 - own // 2)
        mirrored = (over + 1) * quarter
        homeward = [
            to * quarter + flipped(low, mask)
            for to in (over + 1, over, own + 1 - 2 * (own % 2), own)
            for mask in range(quarter - 1, -1, -1)
        ][:-1]

    loads = []
    for at, (source, target) in enumerate((
        (retarded_hbm.at[0, 0], retarded),
        (lesser_hbm.at[0, 0], lesser),
        (coupling_hbm.at[0], coupling),
        (interaction_hbm.at[0], interaction),
        (forward_hbm, forward),
        (inverse_hbm, inverse),
    )):
        load = pltpu.make_async_copy(source, target, load_sem.at[at])
        loads.append(load)
        if target is coupling:
            pl.when(section > 0)(load.start)
        elif at < 2:
            load.start()

    collects = (me + section // max(last, 1)) % 2 == 1 if split else me >= 0
    barrier = pltpu.get_barrier_semaphore()
    if split:
        for at in range(half):
            peer = 2 * at + 1 - section // last

            @pl.when(peer != me)
            def _():
                pl.semaphore_signal(
                    barrier, inc=1, device_id={"energy": peer}, device_id_type=MESH
                )

        @pl.when(grows)
        def _():
            pl.semaphore_signal(barrier, inc=1, device_id={"space": last}, device_id_type=MESH)
    else:
        for peer in peers:
            pl.semaphore_signal(barrier, inc=1, device_id={"energy": peer}, device_id_type=MESH)

    @pl.when(fed)
    def _():
        pl.semaphore_signal(barrier, inc=1, device_id={"space": section - 1}, device_id_type=MESH)

    def across():
        @pl.when(~collects)
        def _():
            pl.semaphore_wait(barrier, 1)

    def gathered():
        @pl.when(collects)
        def _():
            pl.semaphore_wait(barrier, groups - 1 + jnp.where(feeds, 1, 0))
            if split:
                pl.semaphore_signal(
                    ready, inc=1,
                    device_id={"energy": me + 1 - 2 * (me % 2)}, device_id_type=MESH,
                )

    def told():
        @pl.when(~collects)
        def _():
            pl.semaphore_wait(ready, 1)

        @pl.when(lends)
        def _():
            pl.semaphore_signal(clear, inc=1, device_id={"space": last - 1}, device_id_type=MESH)

    def hop(piece):
        columns = pl.ds(piece * width, width)
        return pltpu.make_async_remote_copy(
            src_ref=green.at[:, :, columns],
            dst_ref=before.at[:, :, columns],
            send_sem=hop_send.at[piece],
            recv_sem=hop_recv.at[piece],
            device_id={"space": section + 1},
            device_id_type=MESH,
        )

    def lend(piece):
        lines = pl.ds(piece * width, width)
        return pltpu.make_async_remote_copy(
            src_ref=maps.at[:, lines, :],
            dst_ref=theirs.at[:, lines, :],
            send_sem=map_send.at[piece],
            recv_sem=map_recv.at[piece],
            device_id={"space": section - 1},
            device_id_type=MESH,
        )

    def make_maps():
        loads[2].wait()
        m_re, m_im = product(retarded[0], retarded[1], coupling[0], coupling[1])
        maps[0], maps[1] = m_re.astype(LOW), m_im.astype(LOW)

    loads[0].wait()

    @pl.when(lends)
    def _():
        make_maps()
        across()
        for piece in range(pieces):
            lend(piece).start()

    loads[1].wait()
    for load in loads[3:]:
        load.start()
    r_re, r_im = retarded[0], retarded[1]
    half_re, half_im = product(r_re, r_im, lesser[0], lesser[1])
    half_re, half_im = half_re.astype(LOW), half_im.astype(LOW)
    total[0], total[1] = product_adjoint(half_re, half_im, r_re, r_im)

    @pl.when(~lends)
    def _():
        across()
        gathered()

    @pl.when(fed)
    def _():
        make_maps()
        for piece in range(pieces):
            hop(piece).wait_recv()
            part = slice(piece * width, (piece + 1) * width)
            k_re, k_im = product(maps[0], maps[1], before[0, :, part], before[1, :, part])
            g_re, g_im = product_adjoint(
                k_re.astype(LOW), k_im.astype(LOW), maps[0, :, part], maps[1, :, part]
            )
            total[0] += g_re
            total[1] += g_im

    @pl.when(feeds | grows)
    def _():
        green[...] = total[...].astype(LOW)

    @pl.when(feeds)
    def _():
        for piece in range(pieces):
            hop(piece).start()

    share = rows // parts

    def entries_of(values, part):
        sides = [
            values[side].reshape(groups, parts, share, order)[:, part] for side in range(2)
        ]
        return beside(*sides, 1)

    def scattered(values, target):
        for part in range(parts):
            target[part] = entries_of(values, part).astype(LOW)

    def go(part, peer, slot):
        return pltpu.make_async_remote_copy(
            src_ref=homing.at[part, peer],
            dst_ref=homed.at[part, slot],
            send_sem=go_send,
            recv_sem=go_recv.at[part],
            device_id={"energy": peer},
            device_id_type=MESH,
        )

    def late(part, peer, slot):
        return pltpu.make_async_remote_copy(
            src_ref=grown.at[part, peer],
            dst_ref=homed.at[part, groups + slot],
            send_sem=late_send,
            recv_sem=late_recv.at[part],
            device_id={"space": last, "energy": peer},
            device_id_type=MESH,
        )

    def pay():
        return pltpu.make_async_remote_copy(
            src_ref=grown.at[direct:],
            dst_ref=repaid,
            send_sem=pay_send,
            recv_sem=pay_recv,
            device_id={"space": last},
            device_id_type=MESH,
        )

    def back(part, peer, slot):
        return pltpu.make_async_remote_copy(
            src_ref=leaving.at[part * groups + peer],
            dst_ref=landed.at[:, slot, part],
            send_sem=back_send,
            recv_sem=back_recv,
            device_id={"energy": peer},
            device_id_type=MESH,
        )

    def drain(ref, sem):
        pltpu.make_async_copy(ref, ref, sem).wait()

    def relay():
        return pltpu.make_async_remote_copy(
            src_ref=leaving.at[pl.ds(mirrored, max(1, quarter))],
            dst_ref=passing,
            send_sem=relay_send,
            recv_sem=relay_recv,
            device_id={"space": last - 1},
            device_id_type=MESH,
        )

    def forward_on(at):
        return pltpu.make_async_remote_copy(
            src_ref=passing.at[at],
            dst_ref=landed.at[:, me, 0],
            send_sem=pass_send,
            recv_sem=back_recv,
            device_id={"space": last, "energy": mirrored + at},
            device_id_type=MESH,
        )

    scattered((total[0], total[1]), homing)
    if split:
        told()

    def send(part):
        for peer in homeward:
            go(part, peer, me).start()
        homed[part, me] = homing[part, me]

    for part in range(parts):
        if split and part >= direct:
            pl.when(~lends)(functools.partial(send, part))
        else:
            send(part)

    if split:
        @pl.when(grows)
        def _():
            for piece in range(pieces):
                lend(piece).wait_recv()
                part = slice(piece * width, (piece + 1) * width)
                k_re, k_im = product(theirs[0, part, :], theirs[1, part, :], green[0], green[1])
                carried[0, part, :], carried[1, part, :] = k_re.astype(LOW), k_im.astype(LOW)
            g_re, g_im = product_adjoint(carried[0], carried[1], theirs[0], theirs[1])
            scattered((g_re, g_im), grown)
            pl.semaphore_wait(clear, 1)
            if direct < parts:
                pay().start()
            for part in range(direct):
                for peer in peers + [me]:
                    late(part, peer, me // 2).start()

        @pl.when(~is_last)
        def _():
            for part in range(direct):
                homed[part, groups:] = jnp.zeros((half, 2 * share, order), LOW)

        if direct < parts:
            @pl.when(lends)
            def _():
                pay().wait_recv()
                for part in range(direct, parts):
                    homing[part] = (
                        entries_of((total[0], total[1]), part)
                        + repaid[part - direct].astype(WIDE)
                    ).astype(LOW)
                    send(part)

    for load in loads[3:]:
        load.wait()

    stride = 2 * length
    chunk = max(1, order // stride)
    for part in range(parts):
        drain(homed.at[part, :groups - 1], go_recv.at[part])
        if split and part < direct:
            @pl.when(is_last)
            def _():
                drain(homed.at[part, groups:], late_recv.at[part])
        count = groups + half if part < direct else groups
        entries = homed[part, :count]
        if 2 * share % 16:
            entries = entries.astype(WIDE)
        entries = entries.reshape(count * 2 * share, order).astype(LOW)
        for first in range(0, share, chunk):
            spectrum = dot(
                forward[first * stride:(first + chunk) * stride, :count * 2 * share], entries
            )
            spectrum = spectrum * groups ** -0.5
            for at in range(chunk):
                row = first + at
                s_re = spectrum[at * stride:at * stride + length]
                s_im = spectrum[at * stride + length:(at + 1) * stride]
                entry = (part * share + row) * order
                weight = interaction[:, entry:entry + order].astype(WIDE)
                weighted[row * stride:row * stride + length, :] = (
                    (s_re * s_re - s_im * s_im) * weight
                ).astype(LOW)
                weighted[row * stride + length:(row + 1) * stride, :] = (
                    2.0 * s_re * s_im * weight
                ).astype(LOW)
        result = dot(inverse[...], weighted[...]) * length ** -0.5
        leaving[part * groups:(part + 1) * groups] = (
            result.reshape(groups, 2, share, order).astype(LOW)
        )
        if split and part == 0:
            @pl.when(grows)
            def _():
                drain(grown.at[:direct], late_send)
                pl.semaphore_signal(turn, inc=1, device_id={"energy": me - 1}, device_id_type=MESH)

            if relays:
                @pl.when(grows & (me // quarter == 1))
                def _():
                    for peer in (me - quarter, me - quarter - 1):
                        pl.semaphore_signal(
                            turn, inc=1, device_id={"energy": peer}, device_id_type=MESH
                        )

                @pl.when(grows & (me // quarter == 0))
                def _():
                    pl.semaphore_wait(turn, 1)

            @pl.when((section == last - 1) & ~odd)
            def _():
                first = me // quarter == 0 if relays else me < 0
                pl.semaphore_wait(turn, jnp.where(first, 2, 1))
        sends = [(part, peer) for peer in homeward]
        if relays:
            upper, lower, near = (
                homeward[:quarter], homeward[quarter:2 * quarter], homeward[2 * quarter:]
            )
            if part == 0:
                @pl.when(is_last)
                def _():
                    relay().start()

                @pl.when(~is_last)
                def _():
                    for peer in upper:
                        back(part, peer, me).start()
            waiting = list(range(1, parts - 1))
            at_last = waiting + [part] if part == parts - 1 else [part]
            if part == 0 or part in waiting:
                at_last = []
            crossing = [(which, peer) for which in at_last for peer in upper]
            home = [(part, peer) for peer in near]
            sends = [(part, peer) for peer in lower] + crossing + home
        for which, peer in sends:
            back(which, peer, me).start()
        landed[:, me, part] = leaving[part * groups + me]

    if relays:
        @pl.when(section == last - 1)
        def _():
            relay().wait_recv()
            for at in range(quarter):
                forward_on(at).start()

    drain(homing.at[:, :groups - 1], go_send)

    @pl.when(feeds)
    def _():
        for piece in range(pieces):
            hop(piece).wait_send()

    if split:
        @pl.when(lends)
        def _():
            for piece in range(pieces):
                lend(piece).wait_send()

        if direct < parts:
            @pl.when(grows)
            def _():
                pay().wait_send()

    if relays:
        @pl.when(section == last - 1)
        def _():
            drain(passing, pass_send)

        @pl.when(is_last)
        def _():
            relay().wait_send()
            drain(leaving.at[:parts * (groups - 1) - quarter], back_send)

        @pl.when(~is_last)
        def _():
            drain(leaving.at[:parts * (groups - 1)], back_send)
    else:
        drain(leaving.at[:parts * (groups - 1)], back_send)
    drain(landed.at[:, :groups - 1], back_recv)


def local(lesser_in, retarded, coupling, interaction):
    order = coupling.shape[-1]
    groups = lax.axis_size("energy")
    sections = lax.axis_size("space")
    length = interaction.shape[1]
    rows = order // groups
    pieces = 2
    parts = 4 if rows % 16 == 0 else 1
    share = rows // parts
    assert lesser_in.shape[0] == 1 and coupling.shape[0] == 1
    late = list(range(1, groups, 2)) if sections > 1 and groups % 2 == 0 else []
    forward = jnp.asarray(forward_matrix(list(range(groups)) + late, length, share))
    inverse = jnp.asarray(inverse_matrix(groups, length, share))
    dma = pltpu.SemaphoreType.DMA
    matrix = (2, order, order)
    spread = (parts, groups, 2 * share, order)
    landed = pl.pallas_call(
        functools.partial(kernel, sections, groups, rows, length, pieces, parts),
        out_shape=pltpu.VMEM((2, groups, parts, share, order), LOW),
        in_specs=[ANY] * 6,
        out_specs=pl.BlockSpec(memory_space=pltpu.VMEM),
        scratch_shapes=[
            pltpu.VMEM(matrix, LOW),
            pltpu.VMEM(matrix, LOW),
            pltpu.VMEM(matrix, LOW),
            pltpu.VMEM(interaction.shape[1:], LOW),
            pltpu.VMEM(forward.shape, LOW),
            pltpu.VMEM(inverse.shape, LOW),
            pltpu.VMEM(matrix, WIDE),
            pltpu.VMEM(matrix, LOW),
            pltpu.VMEM(matrix, LOW),
            pltpu.VMEM(matrix, LOW),
            pltpu.VMEM(matrix, LOW),
            pltpu.VMEM(matrix, LOW),
            pltpu.VMEM(spread, LOW),
            pltpu.VMEM((parts, groups + len(late), 2 * share, order), LOW),
            pltpu.VMEM(spread, LOW),
            pltpu.VMEM((max(1, parts // 4), groups, 2 * share, order), LOW),
            pltpu.VMEM((share * 2 * length, order), LOW),
            pltpu.VMEM((parts * groups, 2, share, order), LOW),
            pltpu.VMEM((max(1, groups // 4), 2, share, order), LOW),
            dma((6,)),
            dma((pieces,)),
            dma((pieces,)),
            dma((pieces,)),
            dma((pieces,)),
            dma,
            dma((parts,)),
            dma,
            dma((parts,)),
            dma,
            dma,
            dma,
            dma,
            dma,
            dma,
            dma,
            pltpu.SemaphoreType.REGULAR,
            pltpu.SemaphoreType.REGULAR,
            pltpu.SemaphoreType.REGULAR,
        ],
        compiler_params=pltpu.CompilerParams(collective_id=0, has_side_effects=True),
    )(lesser_in, retarded, coupling, interaction, forward, inverse)
    return landed.reshape(1, 1, 2, order, order)


def solution(mesh):
    in_specs = (
        P("energy", "space", None, None, None),
        P("energy", "space", None, None, None),
        P("space", None, None, None),
        P("space", None, "energy"),
    )
    out_specs = P("energy", "space", None, None, None)
    return jax.shard_map(local, mesh=mesh, in_specs=in_specs, out_specs=out_specs, check_vma=False)
```

```python
import functools
import math

import jax
import jax.numpy as jnp
import numpy as np
from jax import lax
from jax.experimental import pallas as pl
from jax.experimental.pallas import tpu as pltpu
from jax.sharding import PartitionSpec as P

MESH = pl.DeviceIdType.MESH
ANY = pl.BlockSpec(memory_space=pl.ANY)
LOW, WIDE = jnp.bfloat16, jnp.float32


def phase_parts(row_count, column_count, length):
    residue = np.arange(row_count)[:, None] * np.arange(column_count)[None, :] % length
    phase = residue * (2.0 * math.pi / length)
    return np.cos(phase), np.sin(phase)


def forward_matrix(energies, length, rows):
    cosine, sine = phase_parts(length, max(energies) + 1, length)
    cosine, sine = cosine[:, energies], sine[:, energies]
    small = np.array([[cosine, sine], [-sine, cosine]])
    full = np.einsum("pqfe,rs->rpfeqs", small, np.eye(rows))
    return full.reshape(rows * 2 * length, len(energies) * 2 * rows).astype(LOW)


def inverse_matrix(energy_count, length, rows):
    cosine, sine = phase_parts(energy_count, length, length)
    small = np.array([[cosine, -sine], [sine, cosine]])
    full = np.einsum("pqef,rs->eprsqf", small, np.eye(rows))
    return full.reshape(energy_count * 2 * rows, rows * 2 * length).astype(LOW)


def dot(left, right):
    return jnp.dot(left, right, preferred_element_type=WIDE)


def dot_t(left, right):
    return lax.dot_general(left, right, (((1,), (1,)), ((), ())), preferred_element_type=WIDE)


def product(a_re, a_im, b_re, b_im):
    return dot(a_re, b_re) + dot(-a_im, b_im), dot(a_re, b_im) + dot(a_im, b_re)


def product_adjoint(a_re, a_im, b_re, b_im):
    return dot_t(a_re, b_re) + dot_t(a_im, b_im), dot_t(a_im, b_re) + dot_t(-a_re, b_im)


def beside(first, second, axis):
    return jnp.concatenate([first, second], axis=axis)


def flipped(index, mask):
    bit = 1
    while bit <= mask:
        if mask & bit:
            index = index + bit - 2 * bit * (index // bit % 2)
        bit *= 2
    return index


def kernel(
    sections, groups, rows, length, pieces, parts,
    lesser_hbm, retarded_hbm, coupling_hbm, interaction_hbm, forward_hbm, inverse_hbm,
    landed,
    lesser, retarded, coupling, interaction, forward, inverse,
    total, maps, green, before, theirs, carried, homing, homed, grown, repaid, weighted, leaving, passing,
    load_sem, hop_send, hop_recv, map_send, map_recv, go_send, go_recv, late_send,
    pay_send, pay_recv, back_send, back_recv, relay_send, relay_recv, pass_send, turn, ready, clear,
):
    section = lax.axis_index("space")
    me = lax.axis_index("energy")
    order = green.shape[-1]
    width = order // pieces
    last = sections - 1
    split = sections > 1 and groups % 2 == 0
    half = groups // 2 if split else 0
    direct = parts - parts // 4
    relays = split and groups % 4 == 0 and groups & (groups - 1) == 0
    quarter = groups // 4 if relays else 0
    odd = me % 2 == 1 if split else me < 0
    is_last = section == last
    feeds = (section < last - 1) | ((section == last - 1) & ~odd)
    fed = (section > 0) & ((section < last) | ~odd)
    lends = is_last & odd & (section > 0)
    grows = (section == last - 1) & odd

    if groups & (groups - 1) == 0:
        peers = [flipped(me, mask) for mask in range(groups - 1, 0, -1)]
    else:
        peers = [lax.rem(me + step, groups) for step in range(1, groups)]
    homeward, mirrored = peers, 0
    if relays:
        own, low = me // quarter, me % quarter
        over = 2 * (1 - own // 2)
        mirrored = (over + 1) * quarter
        homeward = [
            to * quarter + flipped(low, mask)
            for to in (over + 1, over, own + 1 - 2 * (own % 2), own)
            for mask in range(quarter - 1, -1, -1)
        ][:-1]

    loads = []
    for at, (source, target) in enumerate((
        (retarded_hbm.at[0, 0], retarded),
        (lesser_hbm.at[0, 0], lesser),
        (coupling_hbm.at[0], coupling),
        (interaction_hbm.at[0], interaction),
        (forward_hbm, forward),
        (inverse_hbm, inverse),
    )):
        load = pltpu.make_async_copy(source, target, load_sem.at[at])
        loads.append(load)
        if target is coupling:
            pl.when(section > 0)(load.start)
        elif at < 2:
            load.start()

    collects = (me + section // max(last, 1)) % 2 == 1 if split else me >= 0
    barrier = pltpu.get_barrier_semaphore()
    if split:
        for at in range(half):
            peer = 2 * at + 1 - section // last

            @pl.when(peer != me)
            def _():
                pl.semaphore_signal(
                    barrier, inc=1, device_id={"energy": peer}, device_id_type=MESH
                )

        @pl.when(grows)
        def _():
            pl.semaphore_signal(barrier, inc=1, device_id={"space": last}, device_id_type=MESH)
    else:
        for peer in peers:
            pl.semaphore_signal(barrier, inc=1, device_id={"energy": peer}, device_id_type=MESH)

    @pl.when(fed)
    def _():
        pl.semaphore_signal(barrier, inc=1, device_id={"space": section - 1}, device_id_type=MESH)

    def across():
        @pl.when(~collects)
        def _():
            pl.semaphore_wait(barrier, 1)

    def gathered():
        @pl.when(collects)
        def _():
            pl.semaphore_wait(barrier, groups - 1 + jnp.where(feeds, 1, 0))
            if split:
                pl.semaphore_signal(
                    ready, inc=1,
                    device_id={"energy": me + 1 - 2 * (me % 2)}, device_id_type=MESH,
                )

    def told():
        @pl.when(~collects)
        def _():
            pl.semaphore_wait(ready, 1)

        @pl.when(lends)
        def _():
            pl.semaphore_signal(clear, inc=1, device_id={"space": last - 1}, device_id_type=MESH)

    def hop(piece):
        columns = pl.ds(piece * width, width)
        return pltpu.make_async_remote_copy(
            src_ref=green.at[:, :, columns],
            dst_ref=before.at[:, :, columns],
            send_sem=hop_send.at[piece],
            recv_sem=hop_recv.at[piece],
            device_id={"space": section + 1},
            device_id_type=MESH,
        )

    def lend(piece):
        lines = pl.ds(piece * width, width)
        return pltpu.make_async_remote_copy(
            src_ref=maps.at[:, lines, :],
            dst_ref=theirs.at[:, lines, :],
            send_sem=map_send.at[piece],
            recv_sem=map_recv.at[piece],
            device_id={"space": section - 1},
            device_id_type=MESH,
        )

    def make_maps():
        loads[2].wait()
        m_re, m_im = product(retarded[0], retarded[1], coupling[0], coupling[1])
        maps[0], maps[1] = m_re.astype(LOW), m_im.astype(LOW)

    loads[0].wait()

    @pl.when(lends)
    def _():
        make_maps()
        across()
        for piece in range(pieces):
            lend(piece).start()

    loads[1].wait()
    for load in loads[3:]:
        load.start()
    r_re, r_im = retarded[0], retarded[1]
    half_re, half_im = product(r_re, r_im, lesser[0], lesser[1])
    half_re, half_im = half_re.astype(LOW), half_im.astype(LOW)
    total[0], total[1] = product_adjoint(half_re, half_im, r_re, r_im)

    @pl.when(~lends)
    def _():
        across()
        gathered()

    @pl.when(fed)
    def _():
        make_maps()
        for piece in range(pieces):
            hop(piece).wait_recv()
            part = slice(piece * width, (piece + 1) * width)
            k_re, k_im = product(maps[0], maps[1], before[0, :, part], before[1, :, part])
            g_re, g_im = product_adjoint(
                k_re.astype(LOW), k_im.astype(LOW), maps[0, :, part], maps[1, :, part]
            )
            total[0] += g_re
            total[1] += g_im

    @pl.when(feeds | grows)
    def _():
        green[...] = total[...].astype(LOW)

    @pl.when(feeds)
    def _():
        for piece in range(pieces):
            hop(piece).start()

    share = rows // parts

    def entries_of(values, part):
        sides = [
            values[side].reshape(groups, parts, share, order)[:, part] for side in range(2)
        ]
        return beside(*sides, 1)

    def scattered(values, target):
        for part in range(parts):
            target[part] = entries_of(values, part).astype(LOW)

    def go(part, peer, slot):
        return pltpu.make_async_remote_copy(
            src_ref=homing.at[part, peer],
            dst_ref=homed.at[part, slot],
            send_sem=go_send,
            recv_sem=go_recv.at[part],
            device_id={"energy": peer},
            device_id_type=MESH,
        )

    def late(part, peer, slot):
        return pltpu.make_async_remote_copy(
            src_ref=grown.at[part, peer],
            dst_ref=homed.at[part, groups + slot],
            send_sem=late_send,
            recv_sem=go_recv.at[part],
            device_id={"space": last, "energy": peer},
            device_id_type=MESH,
        )

    def pay():
        return pltpu.make_async_remote_copy(
            src_ref=grown.at[direct:],
            dst_ref=repaid,
            send_sem=pay_send,
            recv_sem=pay_recv,
            device_id={"space": last},
            device_id_type=MESH,
        )

    def back(part, peer, slot):
        return pltpu.make_async_remote_copy(
            src_ref=leaving.at[part * groups + peer],
            dst_ref=landed.at[:, slot, part],
            send_sem=back_send,
            recv_sem=back_recv,
            device_id={"energy": peer},
            device_id_type=MESH,
        )

    def drain(ref, sem):
        pltpu.make_async_copy(ref, ref, sem).wait()

    def relay():
        return pltpu.make_async_remote_copy(
            src_ref=leaving.at[pl.ds(mirrored, max(1, quarter))],
            dst_ref=passing,
            send_sem=relay_send,
            recv_sem=relay_recv,
            device_id={"space": last - 1},
            device_id_type=MESH,
        )

    def forward_on(at):
        return pltpu.make_async_remote_copy(
            src_ref=passing.at[at],
            dst_ref=landed.at[:, me, 0],
            send_sem=pass_send,
            recv_sem=back_recv,
            device_id={"space": last, "energy": mirrored + at},
            device_id_type=MESH,
        )

    scattered((total[0], total[1]), homing)
    if split:
        told()

    def send(part):
        for peer in homeward:
            go(part, peer, me).start()
        homed[part, me] = homing[part, me]

    for part in range(parts):
        if split and part >= direct:
            pl.when(~lends)(functools.partial(send, part))
        else:
            send(part)

    if split:
        @pl.when(grows)
        def _():
            for piece in range(pieces):
                lend(piece).wait_recv()
                part = slice(piece * width, (piece + 1) * width)
                k_re, k_im = product(theirs[0, part, :], theirs[1, part, :], green[0], green[1])
                carried[0, part, :], carried[1, part, :] = k_re.astype(LOW), k_im.astype(LOW)
            g_re, g_im = product_adjoint(carried[0], carried[1], theirs[0], theirs[1])
            scattered((g_re, g_im), grown)
            pl.semaphore_wait(clear, 1)
            if direct < parts:
                pay().start()
            for part in range(direct):
                for peer in peers + [me]:
                    late(part, peer, me // 2).start()

        @pl.when(~is_last)
        def _():
            for part in range(direct):
                homed[part, groups:] = jnp.zeros((half, 2 * share, order), LOW)

        if direct < parts:
            @pl.when(lends)
            def _():
                pay().wait_recv()
                for part in range(direct, parts):
                    homing[part] = (
                        entries_of((total[0], total[1]), part)
                        + repaid[part - direct].astype(WIDE)
                    ).astype(LOW)
                    send(part)

    for load in loads[3:]:
        load.wait()

    stride = 2 * length
    chunk = max(1, order // stride)
    for part in range(parts):
        if split and part < direct:
            pl.when(is_last)(
                functools.partial(drain, homed.at[part, :groups + half - 1], go_recv.at[part])
            )
            pl.when(~is_last)(
                functools.partial(drain, homed.at[part, :groups - 1], go_recv.at[part])
            )
        else:
            drain(homed.at[part, :groups - 1], go_recv.at[part])
        count = groups + half if part < direct else groups
        entries = homed[part, :count]
        if 2 * share % 16:
            entries = entries.astype(WIDE)
        entries = entries.reshape(count * 2 * share, order).astype(LOW)
        for first in range(0, share, chunk):
            spectrum = dot(
                forward[first * stride:(first + chunk) * stride, :count * 2 * share], entries
            )
            spectrum = spectrum * groups ** -0.5
            for at in range(chunk):
                row = first + at
                s_re = spectrum[at * stride:at * stride + length]
                s_im = spectrum[at * stride + length:(at + 1) * stride]
                entry = (part * share + row) * order
                weight = interaction[:, entry:entry + order].astype(WIDE)
                weighted[row * stride:row * stride + length, :] = (
                    (s_re * s_re - s_im * s_im) * weight
                ).astype(LOW)
                weighted[row * stride + length:(row + 1) * stride, :] = (
                    2.0 * s_re * s_im * weight
                ).astype(LOW)
        result = dot(inverse[...], weighted[...]) * length ** -0.5
        leaving[part * groups:(part + 1) * groups] = (
            result.reshape(groups, 2, share, order).astype(LOW)
        )
        if split and part == 0:
            @pl.when(grows)
            def _():
                drain(grown.at[:direct], late_send)
                pl.semaphore_signal(turn, inc=1, device_id={"energy": me - 1}, device_id_type=MESH)

            if relays:
                @pl.when(grows & (me // quarter == 1))
                def _():
                    for peer in (me - quarter, me - quarter - 1):
                        pl.semaphore_signal(
                            turn, inc=1, device_id={"energy": peer}, device_id_type=MESH
                        )

                @pl.when(grows & (me // quarter == 0))
                def _():
                    pl.semaphore_wait(turn, 1)

            @pl.when((section == last - 1) & ~odd)
            def _():
                first = me // quarter == 0 if relays else me < 0
                pl.semaphore_wait(turn, jnp.where(first, 2, 1))
        sends = [(part, peer) for peer in homeward]
        if relays:
            upper, lower, near = (
                homeward[:quarter], homeward[quarter:2 * quarter], homeward[2 * quarter:]
            )
            if part == 0:
                @pl.when(is_last)
                def _():
                    relay().start()

                @pl.when(~is_last)
                def _():
                    for peer in upper:
                        back(part, peer, me).start()
            waiting = list(range(1, parts - 1))
            at_last = waiting + [part] if part == parts - 1 else [part]
            if part == 0 or part in waiting:
                at_last = []
            crossing = [(which, peer) for which in at_last for peer in upper]
            home = [(part, peer) for peer in near]
            sends = [(part, peer) for peer in lower] + crossing + home
        for which, peer in sends:
            back(which, peer, me).start()
        landed[:, me, part] = leaving[part * groups + me]

    if relays:
        @pl.when(section == last - 1)
        def _():
            relay().wait_recv()
            for at in range(quarter):
                forward_on(at).start()

    drain(homing.at[:, :groups - 1], go_send)

    @pl.when(feeds)
    def _():
        for piece in range(pieces):
            hop(piece).wait_send()

    if split:
        @pl.when(lends)
        def _():
            for piece in range(pieces):
                lend(piece).wait_send()

        if direct < parts:
            @pl.when(grows)
            def _():
                pay().wait_send()

    if relays:
        @pl.when(section == last - 1)
        def _():
            drain(passing, pass_send)

        @pl.when(is_last)
        def _():
            relay().wait_send()
            drain(leaving.at[:parts * (groups - 1) - quarter], back_send)

        @pl.when(~is_last)
        def _():
            drain(leaving.at[:parts * (groups - 1)], back_send)
    else:
        drain(leaving.at[:parts * (groups - 1)], back_send)
    drain(landed.at[:, :groups - 1], back_recv)


def local(lesser_in, retarded, coupling, interaction):
    order = coupling.shape[-1]
    groups = lax.axis_size("energy")
    sections = lax.axis_size("space")
    length = interaction.shape[1]
    rows = order // groups
    pieces = 1
    parts = 4 if rows % 16 == 0 else 1
    share = rows // parts
    assert lesser_in.shape[0] == 1 and coupling.shape[0] == 1
    late = list(range(1, groups, 2)) if sections > 1 and groups % 2 == 0 else []
    forward = jnp.asarray(forward_matrix(list(range(groups)) + late, length, share))
    inverse = jnp.asarray(inverse_matrix(groups, length, share))
    dma = pltpu.SemaphoreType.DMA
    matrix = (2, order, order)
    spread = (parts, groups, 2 * share, order)
    landed = pl.pallas_call(
        functools.partial(kernel, sections, groups, rows, length, pieces, parts),
        out_shape=pltpu.VMEM((2, groups, parts, share, order), LOW),
        in_specs=[ANY] * 6,
        out_specs=pl.BlockSpec(memory_space=pltpu.VMEM),
        scratch_shapes=[
            pltpu.VMEM(matrix, LOW),
            pltpu.VMEM(matrix, LOW),
            pltpu.VMEM(matrix, LOW),
            pltpu.VMEM(interaction.shape[1:], LOW),
            pltpu.VMEM(forward.shape, LOW),
            pltpu.VMEM(inverse.shape, LOW),
            pltpu.VMEM(matrix, WIDE),
            pltpu.VMEM(matrix, LOW),
            pltpu.VMEM(matrix, LOW),
            pltpu.VMEM(matrix, LOW),
            pltpu.VMEM(matrix, LOW),
            pltpu.VMEM(matrix, LOW),
            pltpu.VMEM(spread, LOW),
            pltpu.VMEM((parts, groups + len(late), 2 * share, order), LOW),
            pltpu.VMEM(spread, LOW),
            pltpu.VMEM((max(1, parts // 4), groups, 2 * share, order), LOW),
            pltpu.VMEM((share * 2 * length, order), LOW),
            pltpu.VMEM((parts * groups, 2, share, order), LOW),
            pltpu.VMEM((max(1, groups // 4), 2, share, order), LOW),
            dma((6,)),
            dma((pieces,)),
            dma((pieces,)),
            dma((pieces,)),
            dma((pieces,)),
            dma,
            dma((parts,)),
            dma,
            dma,
            dma,
            dma,
            dma,
            dma,
            dma,
            dma,
            pltpu.SemaphoreType.REGULAR,
            pltpu.SemaphoreType.REGULAR,
            pltpu.SemaphoreType.REGULAR,
        ],
        compiler_params=pltpu.CompilerParams(collective_id=0, has_side_effects=True),
    )(lesser_in, retarded, coupling, interaction, forward, inverse)
    return landed.reshape(1, 1, 2, order, order)


def solution(mesh):
    in_specs = (
        P("energy", "space", None, None, None),
        P("energy", "space", None, None, None),
        P("space", None, None, None),
        P("space", None, "energy"),
    )
    out_specs = P("energy", "space", None, None, None)
    return jax.shard_map(local, mesh=mesh, in_specs=in_specs, out_specs=out_specs, check_vma=False)
```

```python
import functools
import math

import jax
import jax.numpy as jnp
import numpy as np
from jax import lax
from jax.experimental import pallas as pl
from jax.experimental.pallas import tpu as pltpu
from jax.sharding import PartitionSpec as P

MESH = pl.DeviceIdType.MESH
ANY = pl.BlockSpec(memory_space=pl.ANY)
LOW, WIDE = jnp.bfloat16, jnp.float32


def phase_parts(row_count, column_count, length):
    residue = np.arange(row_count)[:, None] * np.arange(column_count)[None, :] % length
    phase = residue * (2.0 * math.pi / length)
    return np.cos(phase), np.sin(phase)


def forward_matrix(energies, length, rows):
    cosine, sine = phase_parts(length, max(energies) + 1, length)
    cosine, sine = cosine[:, energies], sine[:, energies]
    small = np.array([[cosine, sine], [-sine, cosine]])
    full = np.einsum("pqfe,rs->rpfeqs", small, np.eye(rows))
    return full.reshape(rows * 2 * length, len(energies) * 2 * rows).astype(LOW)


def inverse_matrix(energy_count, length, rows):
    cosine, sine = phase_parts(energy_count, length, length)
    small = np.array([[cosine, -sine], [sine, cosine]])
    full = np.einsum("pqef,rs->eprsqf", small, np.eye(rows))
    return full.reshape(energy_count * 2 * rows, rows * 2 * length).astype(LOW)


def dot(left, right):
    return jnp.dot(left, right, preferred_element_type=WIDE)


def dot_t(left, right):
    return lax.dot_general(left, right, (((1,), (1,)), ((), ())), preferred_element_type=WIDE)


def product(a_re, a_im, b_re, b_im):
    return dot(a_re, b_re) + dot(-a_im, b_im), dot(a_re, b_im) + dot(a_im, b_re)


def product_adjoint(a_re, a_im, b_re, b_im):
    return dot_t(a_re, b_re) + dot_t(a_im, b_im), dot_t(a_im, b_re) + dot_t(-a_re, b_im)


def beside(first, second, axis):
    return jnp.concatenate([first, second], axis=axis)


def flipped(index, mask):
    bit = 1
    while bit <= mask:
        if mask & bit:
            index = index + bit - 2 * bit * (index // bit % 2)
        bit *= 2
    return index


def kernel(
    sections, groups, rows, length, pieces, parts,
    lesser_hbm, retarded_hbm, coupling_hbm, interaction_hbm, forward_hbm, inverse_hbm,
    landed,
    lesser, retarded, coupling, interaction, forward, inverse,
    total, maps, green, before, theirs, carried, homing, homed, grown, repaid, weighted, leaving, passing,
    load_sem, hop_send, hop_recv, map_send, map_recv, go_send, go_recv, late_send, late_recv,
    pay_send, pay_recv, back_send, back_recv, relay_send, relay_recv, pass_send, turn, ready, clear,
):
    section = lax.axis_index("space")
    me = lax.axis_index("energy")
    order = green.shape[-1]
    width = order // pieces
    last = sections - 1
    split = sections > 1 and groups % 2 == 0
    half = groups // 2 if split else 0
    direct = parts - parts // 4
    relays = split and groups % 4 == 0 and groups & (groups - 1) == 0
    quarter = groups // 4 if relays else 0
    odd = me % 2 == 1 if split else me < 0
    is_last = section == last
    feeds = (section < last - 1) | ((section == last - 1) & ~odd)
    fed = (section > 0) & ((section < last) | ~odd)
    lends = is_last & odd & (section > 0)
    grows = (section == last - 1) & odd

    if groups & (groups - 1) == 0:
        peers = [flipped(me, mask) for mask in range(groups - 1, 0, -1)]
    else:
        peers = [lax.rem(me + step, groups) for step in range(1, groups)]
    homeward, mirrored = peers, 0
    if relays:
        own, low = me // quarter, me % quarter
        over = 2 * (1 - own // 2)
        mirrored = (over + 1) * quarter
        homeward = [
            to * quarter + flipped(low, mask)
            for to in (over + 1, over, own + 1 - 2 * (own % 2), own)
            for mask in range(quarter - 1, -1, -1)
        ][:-1]

    loads = []
    for at, (source, target) in enumerate((
        (retarded_hbm.at[0, 0], retarded),
        (lesser_hbm.at[0, 0], lesser),
        (coupling_hbm.at[0], coupling),
        (interaction_hbm.at[0], interaction),
        (forward_hbm, forward),
        (inverse_hbm, inverse),
    )):
        load = pltpu.make_async_copy(source, target, load_sem.at[at])
        loads.append(load)
        if target is coupling:
            pl.when(section > 0)(load.start)
        elif at < 2:
            load.start()

    collects = (me + section // max(last, 1)) % 2 == 1 if split else me >= 0
    barrier = pltpu.get_barrier_semaphore()
    if split:
        for at in range(half):
            peer = 2 * at + 1 - section // last

            @pl.when(peer != me)
            def _():
                pl.semaphore_signal(
                    barrier, inc=1, device_id={"energy": peer}, device_id_type=MESH
                )

        @pl.when(grows)
        def _():
            pl.semaphore_signal(barrier, inc=1, device_id={"space": last}, device_id_type=MESH)
    else:
        for peer in peers:
            pl.semaphore_signal(barrier, inc=1, device_id={"energy": peer}, device_id_type=MESH)

    @pl.when(fed)
    def _():
        pl.semaphore_signal(barrier, inc=1, device_id={"space": section - 1}, device_id_type=MESH)

    def across():
        @pl.when(~collects)
        def _():
            pl.semaphore_wait(barrier, 1)

    def gathered():
        @pl.when(collects)
        def _():
            pl.semaphore_wait(barrier, groups - 1 + jnp.where(feeds, 1, 0))
            if split:
                pl.semaphore_signal(
                    ready, inc=1,
                    device_id={"energy": me + 1 - 2 * (me % 2)}, device_id_type=MESH,
                )

    def told():
        @pl.when(~collects)
        def _():
            pl.semaphore_wait(ready, 1)

        @pl.when(lends)
        def _():
            pl.semaphore_signal(clear, inc=1, device_id={"space": last - 1}, device_id_type=MESH)

    def hop(piece):
        columns = pl.ds(piece * width, width)
        return pltpu.make_async_remote_copy(
            src_ref=green.at[:, :, columns],
            dst_ref=before.at[:, :, columns],
            send_sem=hop_send.at[piece],
            recv_sem=hop_recv.at[piece],
            device_id={"space": section + 1},
            device_id_type=MESH,
        )

    def lend(piece):
        lines = pl.ds(piece * width, width)
        return pltpu.make_async_remote_copy(
            src_ref=maps.at[:, lines, :],
            dst_ref=theirs.at[:, lines, :],
            send_sem=map_send.at[piece],
            recv_sem=map_recv.at[piece],
            device_id={"space": section - 1},
            device_id_type=MESH,
        )

    def make_maps():
        loads[2].wait()
        m_re, m_im = product(retarded[0], retarded[1], coupling[0], coupling[1])
        maps[0], maps[1] = m_re.astype(LOW), m_im.astype(LOW)

    loads[0].wait()

    @pl.when(lends)
    def _():
        make_maps()
        across()
        for piece in range(pieces):
            lend(piece).start()

    loads[1].wait()
    for load in loads[3:]:
        load.start()
    r_re, r_im = retarded[0], retarded[1]
    half_re, half_im = product(r_re, r_im, lesser[0], lesser[1])
    half_re, half_im = half_re.astype(LOW), half_im.astype(LOW)
    total[0], total[1] = product_adjoint(half_re, half_im, r_re, r_im)

    @pl.when(~lends)
    def _():
        across()
        gathered()

    @pl.when(fed)
    def _():
        make_maps()
        for piece in range(pieces):
            hop(piece).wait_recv()
            part = slice(piece * width, (piece + 1) * width)
            k_re, k_im = product(maps[0], maps[1], before[0, :, part], before[1, :, part])
            g_re, g_im = product_adjoint(
                k_re.astype(LOW), k_im.astype(LOW), maps[0, :, part], maps[1, :, part]
            )
            total[0] += g_re
            total[1] += g_im

    @pl.when(feeds | grows)
    def _():
        green[...] = total[...].astype(LOW)

    @pl.when(feeds)
    def _():
        for piece in range(pieces):
            hop(piece).start()

    share = rows // parts

    def entries_of(values, part):
        sides = [
            values[side].reshape(groups, parts, share, order)[:, part] for side in range(2)
        ]
        return beside(*sides, 1)

    def scattered(values, target):
        for part in range(parts):
            target[part] = entries_of(values, part).astype(LOW)

    def go(part, peer, slot):
        return pltpu.make_async_remote_copy(
            src_ref=homing.at[part, peer],
            dst_ref=homed.at[part, slot],
            send_sem=go_send,
            recv_sem=go_recv.at[part],
            device_id={"energy": peer},
            device_id_type=MESH,
        )

    def late(part, peer, slot):
        return pltpu.make_async_remote_copy(
            src_ref=grown.at[part, peer],
            dst_ref=homed.at[part, groups + slot],
            send_sem=late_send,
            recv_sem=late_recv.at[part],
            device_id={"space": last, "energy": peer},
            device_id_type=MESH,
        )

    def pay():
        return pltpu.make_async_remote_copy(
            src_ref=grown.at[direct:],
            dst_ref=repaid,
            send_sem=pay_send,
            recv_sem=pay_recv,
            device_id={"space": last},
            device_id_type=MESH,
        )

    def back(part, peer, slot):
        return pltpu.make_async_remote_copy(
            src_ref=leaving.at[part * groups + peer],
            dst_ref=landed.at[:, slot, part],
            send_sem=back_send,
            recv_sem=back_recv,
            device_id={"energy": peer},
            device_id_type=MESH,
        )

    def drain(ref, sem):
        pltpu.make_async_copy(ref, ref, sem).wait()

    def relay():
        return pltpu.make_async_remote_copy(
            src_ref=leaving.at[pl.ds(mirrored, max(1, quarter))],
            dst_ref=passing,
            send_sem=relay_send,
            recv_sem=relay_recv,
            device_id={"space": last - 1},
            device_id_type=MESH,
        )

    def forward_on(at):
        return pltpu.make_async_remote_copy(
            src_ref=passing.at[at],
            dst_ref=landed.at[:, me, 0],
            send_sem=pass_send,
            recv_sem=back_recv,
            device_id={"space": last, "energy": mirrored + at},
            device_id_type=MESH,
        )

    scattered((total[0], total[1]), homing)
    if split:
        told()

    def send(part):
        for peer in homeward:
            go(part, peer, me).start()
        homed[part, me] = homing[part, me]

    for part in range(parts):
        if split and part >= direct:
            pl.when(~lends)(functools.partial(send, part))
        else:
            send(part)

    if split:
        @pl.when(grows)
        def _():
            for piece in range(pieces):
                lend(piece).wait_recv()
                part = slice(piece * width, (piece + 1) * width)
                k_re, k_im = product(theirs[0, part, :], theirs[1, part, :], green[0], green[1])
                carried[0, part, :], carried[1, part, :] = k_re.astype(LOW), k_im.astype(LOW)
            g_re, g_im = product_adjoint(carried[0], carried[1], theirs[0], theirs[1])
            scattered((g_re, g_im), grown)
            pl.semaphore_wait(clear, 1)
            if direct < parts:
                pay().start()
            for part in range(direct):
                for peer in peers + [me]:
                    late(part, peer, me // 2).start()

        @pl.when(~is_last)
        def _():
            for part in range(direct):
                homed[part, groups:] = jnp.zeros((half, 2 * share, order), LOW)

        if direct < parts:
            @pl.when(lends)
            def _():
                pay().wait_recv()
                for part in range(direct, parts):
                    homing[part] = (
                        entries_of((total[0], total[1]), part)
                        + repaid[part - direct].astype(WIDE)
                    ).astype(LOW)
                    send(part)

    for load in loads[3:]:
        load.wait()

    stride = 2 * length
    chunk = max(1, order // stride)
    for part in range(parts):
        drain(homed.at[part, :groups - 1], go_recv.at[part])
        if split and part < direct:
            @pl.when(is_last)
            def _():
                drain(homed.at[part, groups:], late_recv.at[part])
        count = groups + half if part < direct else groups
        entries = homed[part, :count]
        if 2 * share % 16:
            entries = entries.astype(WIDE)
        entries = entries.reshape(count * 2 * share, order).astype(LOW)
        for first in range(0, share, chunk):
            spectrum = dot(
                forward[first * stride:(first + chunk) * stride, :count * 2 * share], entries
            )
            spectrum = spectrum * groups ** -0.5
            for at in range(chunk):
                row = first + at
                s_re = spectrum[at * stride:at * stride + length]
                s_im = spectrum[at * stride + length:(at + 1) * stride]
                entry = (part * share + row) * order
                weight = interaction[:, entry:entry + order].astype(WIDE)
                weighted[row * stride:row * stride + length, :] = (
                    (s_re * s_re - s_im * s_im) * weight
                ).astype(LOW)
                weighted[row * stride + length:(row + 1) * stride, :] = (
                    2.0 * s_re * s_im * weight
                ).astype(LOW)
        result = dot(inverse[...], weighted[...]) * length ** -0.5
        leaving[part * groups:(part + 1) * groups] = (
            result.reshape(groups, 2, share, order).astype(LOW)
        )
        if split and part == 0:
            @pl.when(grows)
            def _():
                drain(grown.at[:direct], late_send)
                pl.semaphore_signal(turn, inc=1, device_id={"energy": me - 1}, device_id_type=MESH)

            if relays:
                @pl.when(grows & (me // quarter == 1))
                def _():
                    for peer in (me - quarter, me - quarter - 1):
                        pl.semaphore_signal(
                            turn, inc=1, device_id={"energy": peer}, device_id_type=MESH
                        )

                @pl.when(grows & (me // quarter == 0))
                def _():
                    pl.semaphore_wait(turn, 1)

            @pl.when((section == last - 1) & ~odd)
            def _():
                first = me // quarter == 0 if relays else me < 0
                pl.semaphore_wait(turn, jnp.where(first, 2, 1))
        sends = [(part, peer) for peer in homeward]
        if relays:
            upper, lower, near = (
                homeward[:quarter], homeward[quarter:2 * quarter], homeward[2 * quarter:]
            )
            if part == 0:
                @pl.when(is_last)
                def _():
                    relay().start()

            waiting = list(range(1, parts - 1))
            at_last = waiting + [part] if part == parts - 1 else [part]
            if part == 0 or part in waiting:
                at_last = []
            crossing = [(which, peer) for which in at_last for peer in upper]
            home = [(part, peer) for peer in near]
            sends = [(part, peer) for peer in lower] + crossing + home
        for which, peer in sends:
            back(which, peer, me).start()
        if relays and part == parts - 1:
            @pl.when(~is_last)
            def _():
                for peer in homeward[:quarter]:
                    back(0, peer, me).start()
        landed[:, me, part] = leaving[part * groups + me]

    if relays:
        @pl.when(section == last - 1)
        def _():
            relay().wait_recv()
            for at in range(quarter):
                forward_on(at).start()

    drain(homing.at[:, :groups - 1], go_send)

    @pl.when(feeds)
    def _():
        for piece in range(pieces):
            hop(piece).wait_send()

    if split:
        @pl.when(lends)
        def _():
            for piece in range(pieces):
                lend(piece).wait_send()

        if direct < parts:
            @pl.when(grows)
            def _():
                pay().wait_send()

    if relays:
        @pl.when(section == last - 1)
        def _():
            drain(passing, pass_send)

        @pl.when(is_last)
        def _():
            relay().wait_send()
            drain(leaving.at[:parts * (groups - 1) - quarter], back_send)

        @pl.when(~is_last)
        def _():
            drain(leaving.at[:parts * (groups - 1)], back_send)
    else:
        drain(leaving.at[:parts * (groups - 1)], back_send)
    drain(landed.at[:, :groups - 1], back_recv)


def local(lesser_in, retarded, coupling, interaction):
    order = coupling.shape[-1]
    groups = lax.axis_size("energy")
    sections = lax.axis_size("space")
    length = interaction.shape[1]
    rows = order // groups
    pieces = 2
    parts = 4 if rows % 16 == 0 else 1
    share = rows // parts
    assert lesser_in.shape[0] == 1 and coupling.shape[0] == 1
    late = list(range(1, groups, 2)) if sections > 1 and groups % 2 == 0 else []
    forward = jnp.asarray(forward_matrix(list(range(groups)) + late, length, share))
    inverse = jnp.asarray(inverse_matrix(groups, length, share))
    dma = pltpu.SemaphoreType.DMA
    matrix = (2, order, order)
    spread = (parts, groups, 2 * share, order)
    landed = pl.pallas_call(
        functools.partial(kernel, sections, groups, rows, length, pieces, parts),
        out_shape=pltpu.VMEM((2, groups, parts, share, order), LOW),
        in_specs=[ANY] * 6,
        out_specs=pl.BlockSpec(memory_space=pltpu.VMEM),
        scratch_shapes=[
            pltpu.VMEM(matrix, LOW),
            pltpu.VMEM(matrix, LOW),
            pltpu.VMEM(matrix, LOW),
            pltpu.VMEM(interaction.shape[1:], LOW),
            pltpu.VMEM(forward.shape, LOW),
            pltpu.VMEM(inverse.shape, LOW),
            pltpu.VMEM(matrix, WIDE),
            pltpu.VMEM(matrix, LOW),
            pltpu.VMEM(matrix, LOW),
            pltpu.VMEM(matrix, LOW),
            pltpu.VMEM(matrix, LOW),
            pltpu.VMEM(matrix, LOW),
            pltpu.VMEM(spread, LOW),
            pltpu.VMEM((parts, groups + len(late), 2 * share, order), LOW),
            pltpu.VMEM(spread, LOW),
            pltpu.VMEM((max(1, parts // 4), groups, 2 * share, order), LOW),
            pltpu.VMEM((share * 2 * length, order), LOW),
            pltpu.VMEM((parts * groups, 2, share, order), LOW),
            pltpu.VMEM((max(1, groups // 4), 2, share, order), LOW),
            dma((6,)),
            dma((pieces,)),
            dma((pieces,)),
            dma((pieces,)),
            dma((pieces,)),
            dma,
            dma((parts,)),
            dma,
            dma((parts,)),
            dma,
            dma,
            dma,
            dma,
            dma,
            dma,
            dma,
            pltpu.SemaphoreType.REGULAR,
            pltpu.SemaphoreType.REGULAR,
            pltpu.SemaphoreType.REGULAR,
        ],
        compiler_params=pltpu.CompilerParams(collective_id=0, has_side_effects=True),
    )(lesser_in, retarded, coupling, interaction, forward, inverse)
    return landed.reshape(1, 1, 2, order, order)


def solution(mesh):
    in_specs = (
        P("energy", "space", None, None, None),
        P("energy", "space", None, None, None),
        P("space", None, None, None),
        P("space", None, "energy"),
    )
    out_specs = P("energy", "space", None, None, None)
    return jax.shard_map(local, mesh=mesh, in_specs=in_specs, out_specs=out_specs, check_vma=False)
```
